16 devices in a mesh: rep: 1, dp: 16 (over x, y, z, core).
Axes of the slice: x: 2, y: 2, z: 2, core: 2. Of those that a mesh axis runs over, the one named last changes fastest.
Arguments:
- x: bfloat16 [16, 2048, 896], P(('rep', 'dp'))
- dy: bfloat16 [16, 2048, 896], P(('rep', 'dp'))
- w_gate: bfloat16 [2, 896, 3584], replicated
- w_up: bfloat16 [2, 896, 3584], replicated
- w_down: bfloat16 [2, 3584, 896], replicated
- m_w_gate: float32 [2, 896, 3584], P(None, 'dp')
- m_w_up: float32 [2, 896, 3584], P(None, 'dp')
- m_w_down: float32 [2, 3584, 896], P(None, 'dp')
- v_w_gate: float32 [2, 896, 3584], P(None, 'dp')
- v_w_up: float32 [2, 896, 3584], P(None, 'dp')
- v_w_down: float32 [2, 3584, 896], P(None, 'dp')
Outputs:
- output 1: bfloat16 [2, 896, 3584], P('rep')
- output 2: bfloat16 [2, 896, 3584], P('rep')
- output 3: bfloat16 [2, 3584, 896], P('rep')
- output 4: float32 [2, 896, 3584], P('rep', 'dp')
- output 5: float32 [2, 896, 3584], P('rep', 'dp')
- output 6: float32 [2, 3584, 896], P('rep', 'dp')
- output 7: float32 [2, 896, 3584], P('rep', 'dp')
- output 8: float32 [2, 896, 3584], P('rep', 'dp')
- output 9: float32 [2, 3584, 896], P('rep', 'dp')
All inputs are finite; a program needn't handle non-finite values.
Results may differ from the reference program's by a relative error of at most 0.022.
Values are sent between devices in bfloat16 or wider.
A program may use at most 2 GiB of HBM per device.

```python
import jax
import jax.numpy as jnp
from jax import lax

SEQUENCES = 16
TOKENS = 2048
D = 896
FF = 3584
LAYERS = 2
NAMES = ("w_gate", "w_up", "w_down")
SHAPES = {"w_gate": (LAYERS, D, FF), "w_up": (LAYERS, D, FF), "w_down": (LAYERS, FF, D)}


def bump(key, n, height):
    away = (jnp.arange(n, dtype=jnp.int32) - jax.random.randint(key, (), 0, n, jnp.int32)) % n
    return jnp.where(away < n // 8, height, 1.0)


def together(key, own, strength):
    shared = jax.random.normal(key, own.shape[1:], jnp.float32)
    return (own + strength * shared) * lax.rsqrt(1 + strength * strength)


def setup_inputs(seed: int = 0, part: int = 0) -> dict:
    kx, kdy, ka, kb, kz, kf, kh, kl, *keys = jax.random.split(jax.random.key(seed), 8 + 3 * len(NAMES))
    kx, kdy, ka, kb = (jax.random.fold_in(k, part) for k in (kx, kdy, ka, kb))
    kw, km, kv = (keys[i::3] for i in range(3))
    shape = (SEQUENCES, TOKENS, D)
    much_x, much_dy = jax.random.uniform(kz, (2,), jnp.float32, 0.0, 1.0)
    loud = 2.0 ** jax.random.uniform(jax.random.fold_in(kz, 1), (), jnp.float32, -1.0, 2.0)
    layers = 2.0 ** jax.random.uniform(kl, (LAYERS, 1, 1), jnp.float32, -1.0, 1.0)
    x = together(ka, jax.random.normal(kx, shape, jnp.float32), much_x) * bump(kf, D, 4.0)
    dy = together(kb, jax.random.normal(kdy, shape, jnp.float32), much_dy)
    drawn = {"x": x.astype(jnp.bfloat16), "dy": (loud * dy * (SEQUENCES * TOKENS) ** -0.5).astype(jnp.bfloat16)}
    for key, name in zip(kw, NAMES, strict=True):
        w = jax.random.normal(key, SHAPES[name], jnp.float32) * SHAPES[name][1] ** -0.5
        drawn[name] = (w * {"w_gate": 1.0, "w_up": bump(kh, FF, 4.0), "w_down": layers}[name]).astype(jnp.bfloat16)
    for key, name in zip(km, NAMES, strict=True):
        drawn[f"m_{name}"] = 0.1 * jax.random.normal(key, SHAPES[name], jnp.float32)
    for key, name in zip(kv, NAMES, strict=True):
        drawn[f"v_{name}"] = jax.random.uniform(key, SHAPES[name], jnp.float32, 0.005, 0.015)
    return drawn


def matmul(a, w):
    return jnp.dot(a, w, preferred_element_type=jnp.float32).astype(jnp.bfloat16)


def normed(h):
    wide = h.astype(jnp.float32)
    scale = lax.rsqrt(jnp.mean(wide**2, -1, keepdims=True) + 1e-6)
    return (wide * scale).astype(jnp.bfloat16)


def layer(h, w):
    a = normed(h)
    gate = jnp.dot(a, w["w_gate"], preferred_element_type=jnp.float32)
    up = jnp.dot(a, w["w_up"], preferred_element_type=jnp.float32)
    return h + matmul((jax.nn.silu(gate) * up).astype(jnp.bfloat16), w["w_down"])


def adamw(w, m, v, g):
    m = 0.9 * m + 0.1 * g
    v = 0.95 * v + 0.05 * g * g
    step = m * lax.rsqrt(v + 1e-8) + 0.1 * w
    return (w - 0.02 * step).astype(jnp.bfloat16), m, v


def stack(weights, h):
    return lax.scan(lambda h, w: (layer(h, w), None), h, weights)[0]


def reference(x, dy, w_gate, w_up, w_down, m_w_gate, m_w_up, m_w_down, v_w_gate, v_w_up, v_w_down):
    weights = dict(zip(NAMES, (w_gate, w_up, w_down), strict=True))

    def take(so_far, sequence):
        h, by_y = sequence
        _, back = jax.vjp(lambda w: stack(w, h), weights)
        return jax.tree.map(lambda total, term: total + term.astype(jnp.float32), so_far, back(by_y)[0]), None

    none_yet = {name: jnp.zeros(w.shape, jnp.float32) for name, w in weights.items()}
    by_weights, _ = lax.scan(take, none_yet, (x, dy))
    gradients = [by_weights[name].astype(jnp.bfloat16).astype(jnp.float32) for name in NAMES]
    new = [
        adamw(w.astype(jnp.float32), m, v, g)
        for w, m, v, g in zip((w_gate, w_up, w_down), (m_w_gate, m_w_up, m_w_down), (v_w_gate, v_w_up, v_w_down), gradients, strict=True)
    ]
    return tuple(one[which] for which in range(3) for one in new)
```

```python
import functools

import jax
import jax.numpy as jnp
from jax import lax
from jax.experimental import pallas as pl
from jax.experimental.pallas import tpu as pltpu
from jax.sharding import PartitionSpec as P


BF, F32 = jnp.bfloat16, jnp.float32
CORE = 1
BIT = {"x": 8, "y": 4, "z": 2}
VMEM = 60 * 2**20


def dot(a, b, ca, cb):
    return lax.dot_general(a, b, (((ca,), (cb,)), ((), ())), preferred_element_type=F32)


def call(kernel, grid, ins, outs, shapes, flops, scratch=(), prefetch=0, aliases={}):
    spec = pltpu.PrefetchScalarGridSpec(
        num_scalar_prefetch=prefetch, grid=grid, in_specs=ins, out_specs=outs, scratch_shapes=scratch
    )
    return pl.pallas_call(
        kernel,
        grid_spec=spec,
        out_shape=shapes,
        input_output_aliases=aliases,
        cost_estimate=pl.CostEstimate(flops=flops, bytes_accessed=flops // 400, transcendentals=0),
        compiler_params=pltpu.CompilerParams(
            vmem_limit_bytes=VMEM, dimension_semantics=("arbitrary",) * len(grid)
        ),
    )


def like(*shapes):
    return [jax.ShapeDtypeStruct(s, d) for s, d in shapes]


def scale_of(wide):
    return lax.rsqrt(jnp.mean(wide**2, -1, keepdims=True) + 1e-6)


def normed(h):
    wide = h.astype(F32)
    return (wide * scale_of(wide)).astype(BF)


def forward(a, w_gate, w_up, n, tile=512):
    t, d = a.shape
    ff = w_gate.shape[2]

    def kernel(a, wg, wu, gate, up, hid):
        g = dot(a[...], wg[...], 1, 0)
        u = dot(a[...], wu[...], 1, 0)
        gate[...] = g
        up[...] = u
        hid[...] = (g * sigmoid(g) * u).astype(BF)

    w = pl.BlockSpec((None, d, tile), lambda j: (n, 0, j))
    o = pl.BlockSpec((t, tile), lambda j: (0, j))
    return call(
        kernel,
        (ff // tile,),
        [pl.BlockSpec((t, d), lambda j: (0, 0)), w, w],
        [o, o, o],
        like(((t, ff), F32), ((t, ff), F32), ((t, ff), BF)),
        4 * t * d * ff,
    )(a, w_gate, w_up)


def down(x, hid, w_down, n, tile=512):
    t, d = x.shape
    ff = hid.shape[1]

    def kernel(x, hid, w, h, a):
        new = x[...].astype(F32) + dot(hid[...], w[...], 1, 0).astype(BF).astype(F32)
        new = new.astype(BF)
        h[...] = new
        a[...] = normed(new)

    o = pl.BlockSpec((tile, d), lambda i: (i, 0))
    return call(
        kernel,
        (t // tile,),
        [o, pl.BlockSpec((tile, ff), lambda i: (i, 0)), pl.BlockSpec((None, ff, d), lambda i: (n, 0, 0))],
        [o, o],
        like(((t, d), BF), ((t, d), BF)),
        2 * t * d * ff,
    )(x, hid, w_down)


def sigmoid(x):
    return 0.5 * jnp.tanh(0.5 * x) + 0.5


def gated_back(g, u, d_hid):
    d_hid = d_hid.astype(BF).astype(F32)
    s = sigmoid(g)
    act = g * s
    d_up = (d_hid * act).astype(BF)
    d_gate = (d_hid * u * (s + act * (1 - s))).astype(BF)
    return act, d_gate, d_up


def turn(a, back, w_gate, w_up, w_down, n, tile=256):
    t, d = a.shape
    ff = w_gate.shape[2]

    def kernel(a, back, wg, wu, wd, hid, d_gate, d_up):
        for r in range(0, t, 512):
            r = slice(r, r + 512)
            g = dot(a[r], wg[...], 1, 0)
            u = dot(a[r], wu[...], 1, 0)
            act, d_gate[r], d_up[r] = gated_back(g, u, dot(back[r], wd[...], 1, 1))
            hid[r] = (act * u).astype(BF)

    whole = pl.BlockSpec((t, d), lambda j: (0, 0))
    w = pl.BlockSpec((None, d, tile), lambda j: (n, 0, j))
    o = pl.BlockSpec((t, tile), lambda j: (0, j))
    return call(
        kernel,
        (ff // tile,),
        [whole, whole, w, w, pl.BlockSpec((None, tile, d), lambda j: (n, j, 0))],
        [o, o, o],
        like(*[((t, ff), BF)] * 3),
        6 * t * d * ff,
    )(a, back, w_gate, w_up, w_down)


def backward(back, gate, up, w_down, n, first, steps, onto=(), tile=512):
    t, d = back.shape
    ff = gate.shape[1]

    def kernel(back, wd, g, u, *refs):
        d_gate, d_up = refs[-2:]
        _, d_gate[...], d_up[...] = gated_back(g[...], u[...], dot(back[...], wd[...], 1, 1))

    o = pl.BlockSpec((t, tile), lambda j: (0, first + j))
    return call(
        kernel,
        (steps,),
        [
            pl.BlockSpec((t, d), lambda j: (0, 0)),
            pl.BlockSpec((None, tile, d), lambda j: (n, first + j, 0)),
            o,
            o,
            *[pl.BlockSpec(memory_space=pl.ANY) for _ in onto],
        ],
        [o, o],
        like(*[((t, ff), BF)] * 2),
        2 * t * d * tile * steps,
        aliases={4: 0, 5: 1} if onto else {},
    )(back, w_down, gate, up, *onto)


def through(d_gate, d_up, w_gate, w_up, h, back, n, half, onto=None, tile=512):
    t, d = h.shape
    ff = d_gate.shape[1]

    def kernel(dg, du, wg, wu, h, back, *refs):
        out = refs[-1]
        d_a = dot(dg[...], wg[...], 1, 1).astype(BF).astype(F32) + dot(du[...], wu[...], 1, 1).astype(BF).astype(F32)
        d_a = d_a.astype(BF).astype(F32)
        wide = h[...].astype(F32)
        scale = scale_of(wide)
        along = jnp.mean(d_a * wide, -1, keepdims=True)
        d_h = scale * d_a - wide * (scale**3 * along)
        out[...] = (back[...].astype(F32) + d_h.astype(BF).astype(F32)).astype(BF)

    steps = t // tile // 2
    o = pl.BlockSpec((tile, d), lambda i: (i + half * steps, 0))
    wide = pl.BlockSpec((tile, ff), lambda i: (i + half * steps, 0))
    w = pl.BlockSpec((None, d, ff), lambda i: (n, 0, 0))
    more = [] if onto is None else [onto]
    return call(
        kernel,
        (steps,),
        [wide, wide, w, w, o, o, *[pl.BlockSpec(memory_space=pl.ANY) for _ in more]],
        o,
        like(((t, d), BF))[0],
        2 * t * d * ff,
        aliases={6: 0} if more else {},
    )(d_gate, d_up, w_gate, w_up, h, back, *more)


def by_columns(me, a, b, tile=512):
    t, d = a.shape
    ff = b.shape[1]
    rows = d // 16

    def kernel(me, a, b, keep, send, acc):
        acc[...] = dot(a[...], b[...], 0, 0).reshape(acc.shape)
        for j in range(8):
            keep[j] = acc[(2 * j) ^ me[0]].astype(BF)
            send[j] = acc[(2 * j + 1) ^ me[0]].astype(BF)

    o = pl.BlockSpec((8, rows, tile), lambda j, me: (0, 0, j))
    return call(
        kernel,
        (ff // tile,),
        [pl.BlockSpec((t, d), lambda j, me: (0, 0)), pl.BlockSpec((t, tile), lambda j, me: (0, j))],
        [o, o],
        like(*[((8, rows, ff), BF)] * 2),
        2 * t * d * ff,
        scratch=[pltpu.VMEM((16, rows, tile), F32)],
        prefetch=1,
    )(me, a, b)


def by_rows(me, a, b):
    t, ff = a.shape
    d = b.shape[1]
    rows = ff // 16

    def kernel(me, a, b, keep, send, acc):
        acc[...] = dot(a[...], b[...], 0, 0).reshape(acc.shape)
        low = me[0] & 3
        for j in range(2):
            keep[j] = acc[(2 * j) ^ low].astype(BF)
            send[j] = acc[(2 * j + 1) ^ low].astype(BF)

    o = pl.BlockSpec((2, rows, d), lambda i, me: (i ^ (me[0] >> 2), 0, 0))
    return call(
        kernel,
        (4,),
        [pl.BlockSpec((t, ff // 4), lambda i, me: (0, i)), pl.BlockSpec((t, d), lambda i, me: (0, 0))],
        [o, o],
        like(*[((8, rows, d), BF)] * 2),
        2 * t * d * ff,
        scratch=[pltpu.VMEM((4, rows, d), F32)],
        prefetch=1,
    )(me, a, b)


def swap(t, bit):
    return lax.ppermute(t, "dp", [(i, i ^ bit) for i in range(16)])


def add(terms):
    return functools.reduce(jnp.add, [t.astype(F32) for t in terms]).astype(BF)


def scattered(keep, send, pieces):
    got = swap(send, CORE)
    out = []
    for start, stop, order in pieces:
        terms = [t.reshape(2, 2, 2, *t.shape[1:])[..., start:stop] for t in (keep, got)]
        left = "xyz"
        for axis in order:
            k = left.index(axis)
            left = left.replace(axis, "")
            near, far = ([lax.index_in_dim(t, side, k, keepdims=False) for t in terms] for side in (0, 1))
            sent = add(far)
            terms = [*near, swap(sent, BIT[axis])]
        out.append(add(terms))
    return out


def gathered(block, order):
    held = block[None]
    for axis in reversed(order):
        got = swap(held, BIT[axis])
        held = jnp.concatenate([held, got])
    return held, swap(held, CORE)


def put(full, n, layers, onto):
    rows, width = full.shape[0] // 16, full.shape[1]

    def kernel(full, *refs):
        refs[-1][...] = full[...]

    more = [] if onto is None else [onto]
    return call(
        kernel,
        (4,),
        [pl.BlockSpec((2, 2, rows, width), lambda k: (k, 0, 0, 0)), *[pl.BlockSpec(memory_space=pl.ANY) for _ in more]],
        pl.BlockSpec((None, 2, 2, rows, width), lambda k: (n, k, 0, 0, 0)),
        like(((layers, 8, 2, rows, width), BF))[0],
        10**9,
        aliases={1: 0} if more else {},
    )(full.reshape(8, 2, rows, width), *more)


def placed(parts, pieces, n, onto):
    _, _, _, rows, width = onto.shape
    flat = [t for both in parts for t in both]

    def kernel(*refs):
        out, held, came, went = refs[-4:]
        me = lax.axis_index("dp")
        core, pair = me & 1, me >> 1

        def copies(j):
            bits = {"x": j >> 2, "y": (j >> 1) & 1, "z": j & 1}
            k = pair ^ j
            for i, (start, stop, order) in enumerate(pieces):
                at = bits[order[0]] * 4 + bits[order[1]] * 2 + bits[order[2]]
                for side in range(2):
                    yield pltpu.make_async_copy(
                        refs[2 * i + side].at[at],
                        held.at[k, core ^ side, :, start:stop],
                        came.at[j, 2 * i + side],
                    )

        def leave(j):
            k = pair ^ j
            return pltpu.make_async_copy(held.at[k], out.at[n, k], went.at[j])

        for j in range(8):
            for copy in copies(j):
                copy.start()
        for j in range(8):
            for copy in copies(j):
                copy.wait()
            leave(j).start()
        for j in range(8):
            leave(j).wait()

    whole = pl.BlockSpec(memory_space=pl.ANY)
    return pl.pallas_call(
        kernel,
        in_specs=[whole] * (len(flat) + 1),
        out_specs=whole,
        out_shape=jax.ShapeDtypeStruct(onto.shape, BF),
        input_output_aliases={len(flat): 0},
        scratch_shapes=[
            pltpu.VMEM((8, 2, rows, width), BF),
            pltpu.SemaphoreType.DMA((8, 2 * len(parts))),
            pltpu.SemaphoreType.DMA((8,)),
        ],
        cost_estimate=pl.CostEstimate(flops=10**9, bytes_accessed=10**7, transcendentals=0),
        compiler_params=pltpu.CompilerParams(vmem_limit_bytes=VMEM),
        name="placed",
    )(*flat, onto)


def adamw(w, m, v, g):
    m = 0.9 * m + 0.1 * g
    v = 0.95 * v + 0.05 * g * g
    step = m * lax.rsqrt(v + 1e-8) + 0.1 * w
    return (w - 0.02 * step).astype(BF), m, v


def solution(mesh):
    ORDERS = ("xyz", "yzx", "zxy")

    def body(x, dy, w_gate, w_up, w_down, *moments):
        x, dy = x[0], dy[0]
        m, v = moments[:3], moments[3:]
        me = lax.axis_index("dp")
        at = me.astype(jnp.int32)[None]
        weights = (w_gate, w_up, w_down)
        new = [[None] * 2 for _ in range(9)]
        whole = [None] * 3

        def pieces_of(which, n):
            width = weights[which].shape[2]
            if n == 1:
                return [(0, width, ORDERS[which])]
            cuts = [0, 1152, 2304, 3584] if width == 3584 else [0, 256, 512, 896]
            return [(cuts[i], cuts[i + 1], ORDERS[(which + i) % 3]) for i in range(3)]

        def update(which, n, keep, send):
            pieces = pieces_of(which, n)
            g = scattered(keep, send, pieces)
            rows = weights[which].shape[1] // 16
            parts, ms, vs = [], [], []
            for (start, stop, order), g in zip(pieces, g, strict=True):
                width = stop - start
                w = lax.dynamic_slice(weights[which], (n, me * rows, start), (1, rows, width))[0].astype(F32)
                w, m2, v2 = adamw(w, m[which][n, :, start:stop], v[which][n, :, start:stop], g.astype(F32))
                ms.append(m2)
                vs.append(v2)
                parts.append(w if n else gathered(w, order))
            new[3 + which][n] = jnp.concatenate(ms, -1)
            new[6 + which][n] = jnp.concatenate(vs, -1)
            if n:
                got = lax.all_gather(parts[0], "dp", axis=0, tiled=True)
                whole[which] = put(got, n, 2, None)
            else:
                whole[which] = placed(parts, pieces, n, whole[which])

        a0 = normed(x)
        gate, up, hid0 = forward(a0, w_gate, w_up, 0)
        h, a1 = down(x, hid0, w_down, 0)
        hid1, d_gate, d_up = turn(a1, dy, w_gate, w_up, w_down, 1)
        update(2, 1, *by_rows(at, hid1, dy))
        update(0, 1, *by_columns(at, a1, d_gate))
        update(1, 1, *by_columns(at, a1, d_up))
        back = through(d_gate, d_up, w_gate, w_up, h, dy, 1, 0)
        back = through(d_gate, d_up, w_gate, w_up, h, dy, 1, 1, back)
        update(2, 0, *by_rows(at, hid0, back))
        d_both = backward(back, gate, up, w_down, 0, 0, 4)
        d_gate, d_up = backward(back, gate, up, w_down, 0, 4, 3, d_both)
        update(0, 0, *by_columns(at, a0, d_gate))
        update(1, 0, *by_columns(at, a0, d_up))
        for i in range(3):
            new[i] = whole[i].reshape(weights[i].shape)
        return tuple(one if i < 3 else jnp.stack(one) for i, one in enumerate(new))

    seq = P(("rep", "dp"), None, None)
    full = P(None, None, None)
    block = P(None, "dp", None)
    return jax.shard_map(
        body,
        mesh=mesh,
        in_specs=(seq, seq, *[full] * 3, *[block] * 6),
        out_specs=(*[P("rep", None, None)] * 3, *[P("rep", "dp", None)] * 6),
        check_vma=False,
    )
```

```python
import jax
import jax.numpy as jnp
from jax import lax
from jax.experimental import pallas as pl
from jax.experimental.pallas import tpu as pltpu
from jax.sharding import PartitionSpec as P

BF, F32 = jnp.bfloat16, jnp.float32
CORE = 1
BIT = {"x": 8, "y": 4, "z": 2}
VMEM = 60 * 2**20


def dot(a, b, ca, cb):
    return lax.dot_general(a, b, (((ca,), (cb,)), ((), ())), preferred_element_type=F32)


def call(kernel, grid, ins, outs, shapes, flops, scratch=(), aliases={}, sums=(), collective_id=None):
    several = isinstance(shapes, list)
    outs, shapes = (outs, shapes) if several else ([outs], [shapes])
    n_in, n_out, n_scratch = len(ins), len(outs), len(scratch)
    hbm = pl.BlockSpec(memory_space=pl.ANY)
    sides, specs, extra, more = [], [], [], []
    for pieces, keep, send, _ in sums:
        rows, width = keep.shape[1:]
        sides += [keep, send]
        specs.append(pl.BlockSpec((rows, width), lambda i: (0, 0)))
        extra.append(jax.ShapeDtypeStruct((rows, width), BF))
        more.append(Side.scratch(pieces, rows))

    def whole(*refs):
        take = iter(refs)
        mine = [[next(take) for _ in range(n)] for n in (n_in, 2 * len(sums), n_out, len(sums), n_scratch)]
        running = [
            Side(one[0], mine[1][2 * k : 2 * k + 2], mine[3][k], [next(take) for _ in more[k]])
            for k, one in enumerate(sums)
        ]
        step = pl.program_id(0)
        for at in sorted({at for one in sums for at in one[3]}):

            @pl.when(step == at)
            def _():
                if at == 0:
                    greet()
                for side, one in zip(running, sums, strict=True):
                    for part, when in enumerate(one[3]):
                        if when == at:
                            side.run(part)

        kernel(*mine[0], *mine[2], *mine[4])
        if sums:

            @pl.when(step == grid[0] - 1)
            def _():
                for side in running:
                    side.end()

    out = pl.pallas_call(
        whole,
        grid=grid,
        in_specs=[*ins, *[hbm] * len(sides)],
        out_specs=[*outs, *specs],
        out_shape=[*shapes, *extra],
        scratch_shapes=[*scratch, *[one for group in more for one in group]],
        input_output_aliases=aliases,
        cost_estimate=pl.CostEstimate(flops=flops, bytes_accessed=flops // 400, transcendentals=0),
        compiler_params=pltpu.CompilerParams(
            vmem_limit_bytes=VMEM,
            dimension_semantics=("arbitrary",) * len(grid),
            collective_id=collective_id,
            has_side_effects=bool(sums),
        ),
    )

    def run(*args):
        got = out(*args, *sides)
        return got if several or sums else got[0]

    return run


def like(*shapes):
    return [jax.ShapeDtypeStruct(s, d) for s, d in shapes]


def scale_of(wide):
    return lax.rsqrt(jnp.mean(wide**2, -1, keepdims=True) + 1e-6)


def normed(h):
    wide = h.astype(F32)
    return (wide * scale_of(wide)).astype(BF)


def forward(a, w_gate, w_up, n, tile=512):
    t, d = a.shape
    ff = w_gate.shape[2]

    def kernel(a, wg, wu, gate, up, hid):
        g = dot(a[...], wg[...], 1, 0)
        u = dot(a[...], wu[...], 1, 0)
        gate[...] = g
        up[...] = u
        hid[...] = (g * sigmoid(g) * u).astype(BF)

    w = pl.BlockSpec((None, d, tile), lambda j: (n, 0, j))
    o = pl.BlockSpec((t, tile), lambda j: (0, j))
    return call(
        kernel,
        (ff // tile,),
        [pl.BlockSpec((t, d), lambda j: (0, 0)), w, w],
        [o, o, o],
        like(((t, ff), F32), ((t, ff), F32), ((t, ff), BF)),
        4 * t * d * ff,
    )(a, w_gate, w_up)


def down(x, hid, w_down, n, tile=512):
    t, d = x.shape
    ff = hid.shape[1]

    def kernel(x, hid, w, h, a):
        new = x[...].astype(F32) + dot(hid[...], w[...], 1, 0).astype(BF).astype(F32)
        new = new.astype(BF)
        h[...] = new
        a[...] = normed(new)

    o = pl.BlockSpec((tile, d), lambda i: (i, 0))
    return call(
        kernel,
        (t // tile,),
        [o, pl.BlockSpec((tile, ff), lambda i: (i, 0)), pl.BlockSpec((None, ff, d), lambda i: (n, 0, 0))],
        [o, o],
        like(((t, d), BF), ((t, d), BF)),
        2 * t * d * ff,
    )(x, hid, w_down)


def sigmoid(x):
    return 0.5 * jnp.tanh(0.5 * x) + 0.5


def gated_back(g, u, d_hid):
    d_hid = d_hid.astype(BF).astype(F32)
    s = sigmoid(g)
    act = g * s
    d_up = (d_hid * act).astype(BF)
    d_gate = (d_hid * u * (s + act * (1 - s))).astype(BF)
    return act, d_gate, d_up


def turn(a, back, w_gate, w_up, w_down, n, tile=256):
    t, d = a.shape
    ff = w_gate.shape[2]

    def kernel(a, back, wg, wu, wd, hid, d_gate, d_up):
        for r in range(0, t, 512):
            r = slice(r, r + 512)
            g = dot(a[r], wg[...], 1, 0)
            u = dot(a[r], wu[...], 1, 0)
            act, d_gate[r], d_up[r] = gated_back(g, u, dot(back[r], wd[...], 1, 1))
            hid[r] = (act * u).astype(BF)

    whole = pl.BlockSpec((t, d), lambda j: (0, 0))
    w = pl.BlockSpec((None, d, tile), lambda j: (n, 0, j))
    o = pl.BlockSpec((t, tile), lambda j: (0, j))
    return call(
        kernel,
        (ff // tile,),
        [whole, whole, w, w, pl.BlockSpec((None, tile, d), lambda j: (n, j, 0))],
        [o, o, o],
        like(*[((t, ff), BF)] * 3),
        6 * t * d * ff,
    )(a, back, w_gate, w_up, w_down)


def backward(back, gate, up, w_down, n, tile=512, sums=(), collective_id=None):
    t, d = back.shape
    ff = gate.shape[1]

    def kernel(back, wd, g, u, d_gate, d_up):
        for r in range(0, t, 512):
            r = slice(r, r + 512)
            _, d_gate[r], d_up[r] = gated_back(g[r], u[r], dot(back[r], wd[...], 1, 1))

    o = pl.BlockSpec((t, tile), lambda j: (0, j))
    return call(
        kernel,
        (ff // tile,),
        [once((t, d), lambda j: (0, 0)), pl.BlockSpec((None, tile, d), lambda j: (n, j, 0)), o, o],
        [o, o],
        like(*[((t, ff), BF)] * 2),
        2 * t * d * ff,
        sums=sums,
        collective_id=collective_id,
    )(back, w_down, gate, up)


def through(d_gate, d_up, w_gate, w_up, h, back, n, tile=256, sums=(), collective_id=None):
    t, d = h.shape
    ff = d_gate.shape[1]

    def kernel(dg, du, wg, wu, h, back, out):
        d_a = dot(dg[...], wg[...], 1, 1).astype(BF).astype(F32) + dot(du[...], wu[...], 1, 1).astype(BF).astype(F32)
        d_a = d_a.astype(BF).astype(F32)
        wide = h[...].astype(F32)
        scale = scale_of(wide)
        along = jnp.mean(d_a * wide, -1, keepdims=True)
        d_h = scale * d_a - wide * (scale**3 * along)
        out[...] = (back[...].astype(F32) + d_h.astype(BF).astype(F32)).astype(BF)

    o = pl.BlockSpec((tile, d), lambda i: (i, 0))
    wide = pl.BlockSpec((tile, ff), lambda i: (i, 0))
    w = once((None, d, ff), lambda i: (n, 0, 0))
    return call(
        kernel,
        (t // tile,),
        [wide, wide, w, w, o, o],
        o,
        like(((t, d), BF))[0],
        4 * t * d * ff,
        sums=sums,
        collective_id=collective_id,
    )(d_gate, d_up, w_gate, w_up, h, back)


def once(shape, index):
    return pl.BlockSpec(shape, index, pipeline_mode=pl.Buffered(1))


def by_columns(a, bs, tile=512, sums=(), collective_id=None):
    t, d = a.shape
    ff = bs[0].shape[1]
    rows, steps = d // 16, ff // tile

    def kernel(a, *refs):
        ins, outs, acc = refs[: len(bs)], refs[len(bs) : -1], refs[-1]
        me = lax.axis_index("dp")
        for k in range(len(bs)):

            @pl.when(pl.program_id(0) // steps == k)
            def _():
                acc[...] = dot(a[...], ins[k][...], 0, 0).reshape(acc.shape)
                for j in range(8):
                    outs[2 * k][j] = acc[(2 * j) ^ me].astype(BF)
                    outs[2 * k + 1][j] = acc[(2 * j + 1) ^ me].astype(BF)

    def at(k):
        return lambda i: jnp.clip(i - k * steps, 0, steps - 1)

    ins = [pl.BlockSpec((t, tile), lambda i, k=k: (0, at(k)(i))) for k in range(len(bs))]
    outs = [pl.BlockSpec((8, rows, tile), lambda i, k=k: (0, 0, at(k)(i))) for k in range(len(bs)) for _ in range(2)]
    return call(
        kernel,
        (steps * len(bs),),
        [once((t, d), lambda i: (0, 0)), *ins],
        outs,
        like(*[((8, rows, ff), BF)] * (2 * len(bs))),
        2 * t * d * ff * len(bs),
        scratch=[pltpu.VMEM((16, rows, tile), F32)],
        sums=sums,
        collective_id=collective_id,
    )(a, *bs)


def by_rows(a, b):
    t, ff = a.shape
    d = b.shape[1]
    rows = ff // 16

    def kernel(a, b, keep, send, acc):
        acc[...] = dot(a[...], b[...], 0, 0).reshape(acc.shape)
        low = lax.axis_index("dp") & 3
        for j in range(2):
            keep[j] = acc[(2 * j) ^ low].astype(BF)
            send[j] = acc[(2 * j + 1) ^ low].astype(BF)

    o = pl.BlockSpec((2, rows, d), lambda i: (i ^ (lax.axis_index("dp") >> 2), 0, 0))
    return call(
        kernel,
        (4,),
        [pl.BlockSpec((t, ff // 4), lambda i: (0, i)), once((t, d), lambda i: (0, 0))],
        [o, o],
        like(*[((8, rows, d), BF)] * 2),
        2 * t * d * ff,
        scratch=[pltpu.VMEM((4, rows, d), F32)],
    )(a, b)


def put(full, n, layers, onto):
    rows, width = full.shape[0] // 16, full.shape[1]

    def kernel(full, *refs):
        refs[-1][...] = full[...]

    more = [] if onto is None else [onto]
    return call(
        kernel,
        (4,),
        [pl.BlockSpec((2, 2, rows, width), lambda k: (k, 0, 0, 0)), *[pl.BlockSpec(memory_space=pl.ANY) for _ in more]],
        pl.BlockSpec((None, 2, 2, rows, width), lambda k: (n, k, 0, 0, 0)),
        like(((layers, 8, 2, rows, width), BF))[0],
        10**9,
        aliases={1: 0} if more else {},
    )(full.reshape(8, 2, rows, width), *more)


def placed(parts, pieces, n, onto):
    _, _, _, rows, width = onto.shape

    def kernel(*refs):
        out, held, came, went = refs[-4:]
        me = lax.axis_index("dp")
        core, pair = me & 1, me >> 1

        def copies(j):
            bits = {"x": j >> 2, "y": (j >> 1) & 1, "z": j & 1}
            k = pair ^ j
            for i, (start, stop, order) in enumerate(pieces):
                at = bits[order[0]] * 4 + bits[order[1]] * 2 + bits[order[2]]
                for side in range(2):
                    yield pltpu.make_async_copy(
                        refs[i].at[8 * side + at],
                        held.at[k, core ^ side, :, start:stop],
                        came.at[j, 2 * i + side],
                    )

        def leave(j):
            k = pair ^ j
            return pltpu.make_async_copy(held.at[k], out.at[n, k], went.at[j])

        for j in range(8):
            for copy in copies(j):
                copy.start()
        for j in range(8):
            for copy in copies(j):
                copy.wait()
            leave(j).start()
        for j in range(8):
            leave(j).wait()

    whole = pl.BlockSpec(memory_space=pl.ANY)
    return pl.pallas_call(
        kernel,
        in_specs=[whole] * (len(parts) + 1),
        out_specs=whole,
        out_shape=jax.ShapeDtypeStruct(onto.shape, BF),
        input_output_aliases={len(parts): 0},
        scratch_shapes=[
            pltpu.VMEM((8, 2, rows, width), BF),
            pltpu.SemaphoreType.DMA((8, 2 * len(parts))),
            pltpu.SemaphoreType.DMA((8,)),
        ],
        cost_estimate=pl.CostEstimate(flops=10**9, bytes_accessed=10**7, transcendentals=0),
        compiler_params=pltpu.CompilerParams(vmem_limit_bytes=VMEM),
        name="placed",
    )(*parts, onto)


BITS = {"x": 4, "y": 2, "z": 1}


def peer(bit):
    return {"dp": lax.axis_index("dp") ^ bit}


def remote(src, dst, sems, i, bit):
    return pltpu.make_async_remote_copy(
        src, dst, sems[0].at[i], sems[1].at[i], device_id=peer(bit), device_id_type=pl.DeviceIdType.MESH
    )


def greet():
    barrier = pltpu.get_barrier_semaphore()
    for bit in (CORE, *BIT.values()):
        pl.semaphore_signal(barrier, inc=1, device_id=peer(bit), device_id_type=pl.DeviceIdType.MESH)
    pl.semaphore_wait(barrier, 4)


class Summed:
    def __init__(self, pieces, refs):
        self.pieces = pieces
        self.mine, self.other = refs[:2]
        self.out = [refs[2 + 3 * i : 5 + 3 * i] for i in range(3)]
        self.got = [refs[11 + 3 * i : 14 + 3 * i] for i in range(3)]
        self.sems = refs[20:22]

    @staticmethod
    def scratch(pieces, rows):
        width = pieces[-1][1]
        whole = [pltpu.VMEM((8, rows, width), BF)] * 2
        halves = [pltpu.VMEM((n, rows, stop - start), BF) for start, stop, _ in pieces for n in (4, 2, 1)]
        return [*whole, *halves, *halves, pltpu.SemaphoreType.DMA((9,)), pltpu.SemaphoreType.DMA((9,))]

    def copy(self, i, stage):
        return remote(self.out[i][stage], self.got[i][stage], self.sems, 3 * i + stage, BIT[self.pieces[i][2][stage]])

    def term(self, i, stage, j):
        start, stop, order = self.pieces[i]
        total = self.mine[j, :, start:stop].astype(F32) + self.other[j, :, start:stop].astype(F32)
        for past in range(stage):
            total = total + self.got[i][past][self.place(order, past, j)].astype(F32)
        return total

    @staticmethod
    def place(order, stage, j):
        rest = [axis for axis in "xyz" if axis not in order[: stage + 1]]
        return sum(bool(j & BITS[axis]) << (len(rest) - 1 - k) for k, axis in enumerate(rest))

    def send(self, stage):
        for i, (_, _, order) in enumerate(self.pieces):
            if stage:
                self.copy(i, stage - 1).wait_recv()
            for j in range(8):
                gone = any(j & BITS[axis] for axis in order[:stage])
                if j & BITS[order[stage]] and not gone:
                    self.out[i][stage][self.place(order, stage, j)] = self.term(i, stage, j).astype(BF)
            self.copy(i, stage).start()

    def total(self, i):
        self.copy(i, 2).wait_recv()
        return self.term(i, 3, 0).astype(BF).astype(F32)

    def finish(self):
        for i in range(3):
            for stage in range(3):
                self.copy(i, stage).wait_send()


class Side:
    def __init__(self, pieces, ins, out, refs):
        self.pieces, self.keep, self.send, self.out = pieces, *ins, out
        self.sum, self.core, self.load = Summed(pieces, refs[:22]), refs[22:24], refs[24]

    @staticmethod
    def scratch(pieces, rows):
        return [*Summed.scratch(pieces, rows), *[pltpu.SemaphoreType.DMA((1,))] * 3]

    def copies(self):
        return (
            pltpu.make_async_copy(self.keep, self.sum.mine, self.load.at[0]),
            remote(self.send, self.sum.other, self.core, 0, CORE),
        )

    def run(self, part):
        if part == 0:
            for copy in self.copies():
                copy.start()
            return
        if part == 1:
            for copy in self.copies():
                copy.wait()
        self.sum.send(part - 1)

    def end(self):
        for i, (start, stop, _) in enumerate(self.pieces):
            self.out[:, start:stop] = self.sum.total(i).astype(BF)
        self.sum.finish()


class Spread:
    def __init__(self, pieces, own, outs, sems):
        self.pieces, self.own, self.outs = pieces, own, outs
        self.sems, self.local = sems[:2], sems[2]

    @staticmethod
    def scratch():
        return [pltpu.SemaphoreType.DMA((21,)), pltpu.SemaphoreType.DMA((21,)), pltpu.SemaphoreType.DMA((3,))]

    def along(self, i, stage):
        n = 1 << stage
        out = self.outs[i]
        src = out.at[pl.ds(0, n)] if stage else self.own[i]
        dst = out.at[pl.ds(n, n)] if stage else out.at[1]
        return remote(src, dst, self.sems, 7 * i + stage, BIT[self.pieces[i][2][2 - stage]])

    def across(self, i, stage):
        out = self.outs[i]
        n = 1 << (stage - 1) if stage else 1
        src = out.at[pl.ds(n, n)] if stage else self.own[i]
        dst = out.at[pl.ds(8 + n, n)] if stage else out.at[8]
        return remote(src, dst, self.sems, 7 * i + 3 + stage, CORE)

    def keep(self, i):
        return pltpu.make_async_copy(self.own[i], self.outs[i].at[0], self.local.at[i])

    def begin(self, i):
        self.along(i, 0).start()
        self.keep(i).start()
        self.across(i, 0).start()

    def step(self, stage):
        for i in range(3):
            self.along(i, stage).wait_recv()
            if stage == 0:
                self.keep(i).wait()
            if stage < 2:
                self.along(i, stage + 1).start()
            self.across(i, stage + 1).start()

    def finish(self):
        for i in range(3):
            for stage in range(3):
                self.along(i, stage).wait_send()
            for stage in range(4):
                self.across(i, stage).wait()


def tail(gate, up, states, pieces):
    rows, width = gate[0].shape[1:]

    def kernel(*refs):
        w_in, m_in, v_in = ((refs[4 + k], refs[7 + k]) for k in range(3))
        outs = [refs[10 + 3 * k : 13 + 3 * k] for k in range(2)]
        m_out, v_out = refs[16:18], refs[18:20]
        sides = [Side(pieces[k], refs[2 * k : 2 * k + 2], None, refs[20 + 25 * k : 45 + 25 * k]) for k in range(2)]
        own = [refs[70:73], refs[73:76]]
        spread = [Spread(pieces[k], own[k], outs[k], refs[76 + 3 * k : 79 + 3 * k]) for k in range(2)]
        greet()
        for part in range(4):
            for side in sides:
                side.run(part)
        for k in range(2):
            for i, (start, stop, _) in enumerate(pieces[k]):
                cols = slice(start, stop)
                new, m_out[k][:, cols], v_out[k][:, cols] = adamw(
                    w_in[k][:, cols].astype(F32), m_in[k][:, cols], v_in[k][:, cols], sides[k].sum.total(i)
                )
                own[k][i][...] = new
                spread[k].begin(i)
        for stage in range(3):
            for k in range(2):
                spread[k].step(stage)
        for k in range(2):
            sides[k].sum.finish()
            spread[k].finish()

    hbm, vmem = pl.BlockSpec(memory_space=pl.ANY), pl.BlockSpec(memory_space=pltpu.VMEM)
    arrays = [jax.ShapeDtypeStruct((16, rows, stop - start), BF) for k in range(2) for start, stop, _ in pieces[k]]
    state = [jax.ShapeDtypeStruct((rows, width), F32)] * 4
    out = pl.pallas_call(
        kernel,
        in_specs=[hbm] * 4 + [vmem] * 6,
        out_specs=[hbm] * 6 + [vmem] * 4,
        out_shape=[*arrays, *state],
        scratch_shapes=[
            *Side.scratch(pieces[0], rows),
            *Side.scratch(pieces[1], rows),
            *[pltpu.VMEM((rows, stop - start), BF) for k in range(2) for start, stop, _ in pieces[k]],
            *Spread.scratch() * 2,
        ],
        cost_estimate=pl.CostEstimate(flops=10**11, bytes_accessed=10**8, transcendentals=0),
        compiler_params=pltpu.CompilerParams(collective_id=1, has_side_effects=True, vmem_limit_bytes=VMEM),
        name="tail",
    )(*gate, *up, *states[0], *states[1])
    return [out[3 * k : 3 * k + 3] for k in range(2)], out[6:8], out[8:10]


def adamw(w, m, v, g):
    m = 0.9 * m + 0.1 * g
    v = 0.95 * v + 0.05 * g * g
    step = m * lax.rsqrt(v + 1e-8) + 0.1 * w
    return (w - 0.02 * step).astype(BF), m, v


def solution(mesh):
    ORDERS = ("xyz", "yzx", "zxy")

    def body(x, dy, w_gate, w_up, w_down, *moments):
        x, dy = x[0], dy[0]
        m, v = moments[:3], moments[3:]
        me = lax.axis_index("dp")
        weights = (w_gate, w_up, w_down)
        new = [[None] * 2 for _ in range(9)]
        whole = [None] * 3

        def pieces_of(which):
            cuts = [0, 256, 512, 896] if which == 2 else [0, 1152, 2304, 3584]
            return [(cuts[i], cuts[i + 1], ORDERS[(which + i) % 3]) for i in range(3)]

        def state(which, n):
            rows, width = weights[which].shape[1] // 16, weights[which].shape[2]
            w = lax.dynamic_slice(weights[which], (n, me * rows, 0), (1, rows, width))[0]
            return w, m[which][n], v[which][n]

        def update(which, n, g):
            w, m1, v1 = state(which, n)
            w, new[3 + which][n], new[6 + which][n] = adamw(w.astype(F32), m1, v1, g.astype(F32))
            whole[which] = put(lax.all_gather(w, "dp", axis=0, tiled=True), n, 2, whole[which])

        a0 = normed(x)
        gate, up, hid0 = forward(a0, w_gate, w_up, 0)
        h, a1 = down(x, hid0, w_down, 0)
        hid1, d_gate, d_up = turn(a1, dy, w_gate, w_up, w_down, 1)
        down1 = by_rows(hid1, dy)
        *both, g = by_columns(a1, (d_gate, d_up), sums=[(pieces_of(2), *down1, (0, 3, 8, 11))], collective_id=2)
        update(2, 1, g)
        sums = [(pieces_of(0), *both[:2], (0, 2, 4, 6)), (pieces_of(1), *both[2:], (0, 3, 5, 7))]
        back, *g = through(d_gate, d_up, w_gate, w_up, h, dy, 1, sums=sums, collective_id=3)
        update(0, 1, g[0])
        update(1, 1, g[1])
        sums = [(pieces_of(2), *by_rows(hid0, back), (0, 2, 4, 5))]
        d_gate, d_up, g = backward(back, gate, up, w_down, 0, sums=sums, collective_id=4)
        update(2, 0, g)
        both = by_columns(a0, (d_gate, d_up))
        pieces = [pieces_of(which) for which in range(2)]
        parts, ms, vs = tail(both[:2], both[2:], (state(0, 0), state(1, 0)), pieces)
        for which in range(2):
            new[3 + which][0], new[6 + which][0] = ms[which], vs[which]
            whole[which] = placed(parts[which], pieces[which], 0, whole[which])
        for i in range(3):
            new[i] = whole[i].reshape(weights[i].shape)
        return tuple(one if i < 3 else jnp.stack(one) for i, one in enumerate(new))

    seq = P(("rep", "dp"), None, None)
    full = P(None, None, None)
    block = P(None, "dp", None)
    return jax.shard_map(
        body,
        mesh=mesh,
        in_specs=(seq, seq, *[full] * 3, *[block] * 6),
        out_specs=(*[P("rep", None, None)] * 3, *[P("rep", "dp", None)] * 6),
        check_vma=False,
    )
```

```python
import jax
import jax.numpy as jnp
from jax import lax
from jax.experimental import pallas as pl
from jax.experimental.pallas import tpu as pltpu
from jax.sharding import PartitionSpec as P

BF, F32 = jnp.bfloat16, jnp.float32
CORE = 1
BIT = {"x": 8, "y": 4, "z": 2}
ALL = (CORE, *BIT.values())
VMEM = 60 * 2**20


def dot(a, b, ca, cb):
    return lax.dot_general(a, b, (((ca,), (cb,)), ((), ())), preferred_element_type=F32)


def call(kernel, grid, ins, outs, shapes, flops, scratch=(), aliases={}, sides=(), collective_id=None, greets=()):
    several = isinstance(shapes, list)
    outs, shapes = (outs, shapes) if several else ([outs], [shapes])
    n_in, n_out, n_scratch = len(ins), len(outs), len(scratch)
    hbm = pl.BlockSpec(memory_space=pl.ANY)
    arrays = [array for side in sides for array in side.arrays]
    results = [one for side in sides for one in side.results()]
    more = [side.scratch() for side in sides]

    def whole(*refs):
        take = iter(refs)

        def some(n):
            return [next(take) for _ in range(n)]

        main = some(n_in)
        given = [some(len(side.arrays)) for side in sides]
        main += some(n_out)
        made = [some(len(side.results())) for side in sides]
        main += some(n_scratch)
        running = [
            side.bind(given[k], made[k], some(len(more[k]))) for k, side in enumerate(sides)
        ]
        step = pl.program_id(0)
        if greets:

            @pl.when(step == 0)
            def _():
                greet(greets)

        for at in sorted({at for side in sides for at, _ in side.plan}):

            @pl.when(step == at)
            def _():
                for side, one in zip(sides, running, strict=True):
                    for when, part in side.plan:
                        if when == at:
                            one.run(part)

        kernel(*main)
        if sides:

            @pl.when(step == grid[0] - 1)
            def _():
                for one in running:
                    one.end()

    out = pl.pallas_call(
        whole,
        grid=grid,
        in_specs=[*ins, *[hbm] * len(arrays)],
        out_specs=[*outs, *[spec for spec, _ in results]],
        out_shape=[*shapes, *[shape for _, shape in results]],
        scratch_shapes=[*scratch, *[one for group in more for one in group]],
        input_output_aliases=aliases,
        cost_estimate=pl.CostEstimate(flops=flops, bytes_accessed=flops // 400, transcendentals=0),
        compiler_params=pltpu.CompilerParams(
            vmem_limit_bytes=VMEM,
            dimension_semantics=("arbitrary",) * len(grid),
            collective_id=collective_id,
            has_side_effects=bool(greets),
        ),
    )

    def run(*args):
        got = out(*args, *arrays)
        return got if several or sides else got[0]

    return run


def size(part):
    return part.stop - part.start


def like(*shapes):
    return [jax.ShapeDtypeStruct(s, d) for s, d in shapes]


def scale_of(wide):
    return lax.rsqrt(jnp.mean(wide**2, -1, keepdims=True) + 1e-6)


def normed(h):
    wide = h.astype(F32)
    return (wide * scale_of(wide)).astype(BF)


def forward(a, w_gate, w_up, n, tile=512):
    t, d = a.shape
    ff = w_gate.shape[2]

    def kernel(a, wg, wu, gate, up, hid):
        g = dot(a[...], wg[...], 1, 0)
        u = dot(a[...], wu[...], 1, 0)
        gate[...] = g
        up[...] = u
        hid[...] = (g * sigmoid(g) * u).astype(BF)

    w = pl.BlockSpec((None, d, tile), lambda j: (n, 0, j))
    o = pl.BlockSpec((t, tile), lambda j: (0, j))
    return call(
        kernel,
        (ff // tile,),
        [pl.BlockSpec((t, d), lambda j: (0, 0)), w, w],
        [o, o, o],
        like(((t, ff), F32), ((t, ff), F32), ((t, ff), BF)),
        4 * t * d * ff,
    )(a, w_gate, w_up)


def down(x, hid, w_down, n, tile=512):
    t, d = x.shape
    ff = hid.shape[1]

    def kernel(x, hid, w, h, a):
        new = x[...].astype(F32) + dot(hid[...], w[...], 1, 0).astype(BF).astype(F32)
        new = new.astype(BF)
        h[...] = new
        a[...] = normed(new)

    o = pl.BlockSpec((tile, d), lambda i: (i, 0))
    return call(
        kernel,
        (t // tile,),
        [o, pl.BlockSpec((tile, ff), lambda i: (i, 0)), pl.BlockSpec((None, ff, d), lambda i: (n, 0, 0))],
        [o, o],
        like(((t, d), BF), ((t, d), BF)),
        2 * t * d * ff,
    )(x, hid, w_down)


def sigmoid(x):
    return 0.5 * jnp.tanh(0.5 * x) + 0.5


def gated_back(g, u, d_hid):
    d_hid = d_hid.astype(BF).astype(F32)
    s = sigmoid(g)
    act = g * s
    d_up = (d_hid * act).astype(BF)
    d_gate = (d_hid * u * (s + act * (1 - s))).astype(BF)
    return act, d_gate, d_up


def turn(a, back, w_gate, w_up, w_down, n, tile=256):
    t, d = a.shape
    ff = w_gate.shape[2]

    def kernel(a, back, wg, wu, wd, hid, d_gate, d_up):
        for r in range(0, t, 512):
            r = slice(r, r + 512)
            g = dot(a[r], wg[...], 1, 0)
            u = dot(a[r], wu[...], 1, 0)
            act, d_gate[r], d_up[r] = gated_back(g, u, dot(back[r], wd[...], 1, 1))
            hid[r] = (act * u).astype(BF)

    whole = pl.BlockSpec((t, d), lambda j: (0, 0))
    w = pl.BlockSpec((None, d, tile), lambda j: (n, 0, j))
    o = pl.BlockSpec((t, tile), lambda j: (0, j))
    return call(
        kernel,
        (ff // tile,),
        [whole, whole, w, w, pl.BlockSpec((None, tile, d), lambda j: (n, j, 0))],
        [o, o, o],
        like(*[((t, ff), BF)] * 3),
        6 * t * d * ff,
    )(a, back, w_gate, w_up, w_down)


def backward(back, gate, up, w_down, n, tile=256, sides=(), collective_id=None):
    t, d = back.shape
    ff = gate.shape[1]

    def kernel(back, wd, g, u, d_gate, d_up):
        for r in range(0, t, 512):
            r = slice(r, r + 512)
            _, d_gate[r], d_up[r] = gated_back(g[r], u[r], dot(back[r], wd[...], 1, 1))

    o = pl.BlockSpec((t, tile), lambda j: (0, j))
    return call(
        kernel,
        (ff // tile,),
        [once((t, d), lambda j: (0, 0)), pl.BlockSpec((None, tile, d), lambda j: (n, j, 0)), o, o],
        [o, o],
        like(*[((t, ff), BF)] * 2),
        2 * t * d * ff,
        sides=sides,
        greets=ALL,
        collective_id=collective_id,
    )(back, w_down, gate, up)


def through(d_gate, d_up, w_gate, w_up, h, back, n, tile=256, sides=(), collective_id=None):
    t, d = h.shape
    ff = d_gate.shape[1]

    def kernel(dg, du, wg, wu, h, back, out):
        d_a = dot(dg[...], wg[...], 1, 1).astype(BF).astype(F32) + dot(du[...], wu[...], 1, 1).astype(BF).astype(F32)
        d_a = d_a.astype(BF).astype(F32)
        wide = h[...].astype(F32)
        scale = scale_of(wide)
        along = jnp.mean(d_a * wide, -1, keepdims=True)
        d_h = scale * d_a - wide * (scale**3 * along)
        out[...] = (back[...].astype(F32) + d_h.astype(BF).astype(F32)).astype(BF)

    o = pl.BlockSpec((tile, d), lambda i: (i, 0))
    wide = pl.BlockSpec((tile, ff), lambda i: (i, 0))
    w = once((None, d, ff), lambda i: (n, 0, 0))
    return call(
        kernel,
        (t // tile,),
        [wide, wide, w, w, o, o],
        o,
        like(((t, d), BF))[0],
        4 * t * d * ff,
        sides=sides,
        greets=ALL,
        collective_id=collective_id,
    )(d_gate, d_up, w_gate, w_up, h, back)


def once(shape, index):
    return pl.BlockSpec(shape, index, pipeline_mode=pl.Buffered(1))


class Crossing:
    def __init__(self, steps, slots, sent, came):
        self.steps, self.slots, self.sems = steps, slots, (sent, came)

    @staticmethod
    def scratch(steps, shape):
        sems = pltpu.SemaphoreType.DMA((steps,))
        return [pltpu.VMEM((2, *shape), BF), sems, sems]

    def copy(self, at, dst):
        return remote(self.slots.at[at % 2], dst, self.sems, at, CORE)

    def slot(self, step, dst):
        @pl.when(step >= 2)
        def _():
            self.copy(step - 2, dst).wait_send()

        return self.slots.at[step % 2]

    def end(self, step, dst):
        @pl.when(step == self.steps - 1)
        def _():
            for at in range(self.steps):
                if at >= self.steps - 2:
                    self.copy(at, dst).wait_send()
                self.copy(at, dst).wait_recv()


def by_columns(a, bs, tile=512, sides=(), collective_id=None):
    t, d = a.shape
    ff = bs[0].shape[1]
    rows, steps = d // 16, ff // tile
    total = steps * len(bs)

    def kernel(a, *refs):
        ins, refs = refs[: len(bs)], refs[len(bs) :]
        kept, got, (acc, *rest) = refs[: len(bs)], refs[len(bs) : 2 * len(bs)], refs[2 * len(bs) :]
        crossing = Crossing(total, *rest)
        me, step = lax.axis_index("dp"), pl.program_id(0)
        slot = crossing.slot(step, got[0].at[:, :, pl.ds(0, tile)])
        for k in range(len(bs)):

            @pl.when(step // steps == k)
            def _():
                acc[...] = dot(a[...], ins[k][...], 0, 0).reshape(acc.shape)
                for j in range(8):
                    slot[j] = acc[(2 * j + 1) ^ me].astype(BF)
                for j in range(8):
                    kept[k][j] = acc[(2 * j) ^ me].astype(BF)
                cols = pl.ds(pl.multiple_of((step - k * steps) * tile, tile), tile)
                crossing.copy(step, got[k].at[:, :, cols]).start()

        crossing.end(step, got[0].at[:, :, pl.ds(0, tile)])

    def at(k):
        return lambda i: jnp.clip(i - k * steps, 0, steps - 1)

    ins = [pl.BlockSpec((t, tile), lambda i, k=k: (0, at(k)(i))) for k in range(len(bs))]
    outs = [pl.BlockSpec((8, rows, tile), lambda i, k=k: (0, 0, at(k)(i))) for k in range(len(bs))]
    return call(
        kernel,
        (total,),
        [once((t, d), lambda i: (0, 0)), *ins],
        [*outs, *[pl.BlockSpec(memory_space=pl.ANY)] * len(bs)],
        like(*[((8, rows, ff), BF)] * (2 * len(bs))),
        2 * t * d * ff * len(bs),
        scratch=[pltpu.VMEM((16, rows, tile), F32), *Crossing.scratch(total, (8, rows, tile))],
        sides=sides,
        collective_id=collective_id,
        greets=ALL,
    )(a, *bs)


def by_rows(a, b, collective_id):
    t, ff = a.shape
    d = b.shape[1]
    rows = ff // 16

    def kernel(a, b, keep, got, acc, *rest):
        crossing = Crossing(4, *rest)
        me, step = lax.axis_index("dp"), pl.program_id(0)
        slot = crossing.slot(step, got.at[pl.ds(0, 2)])
        acc[...] = dot(a[...], b[...], 0, 0).reshape(acc.shape)
        low = me & 3
        for j in range(2):
            slot[j] = acc[(2 * j + 1) ^ low].astype(BF)
        for j in range(2):
            keep[j] = acc[(2 * j) ^ low].astype(BF)
        crossing.copy(step, got.at[pl.ds(2 * (step ^ (me >> 2)), 2)]).start()
        crossing.end(step, got.at[pl.ds(0, 2)])

    return call(
        kernel,
        (4,),
        [pl.BlockSpec((t, ff // 4), lambda i: (0, i)), once((t, d), lambda i: (0, 0))],
        [pl.BlockSpec((2, rows, d), lambda i: (i ^ (lax.axis_index("dp") >> 2), 0, 0)), pl.BlockSpec(memory_space=pl.ANY)],
        like(*[((8, rows, d), BF)] * 2),
        2 * t * d * ff,
        scratch=[pltpu.VMEM((4, rows, d), F32), *Crossing.scratch(4, (2, rows, d))],
        collective_id=collective_id,
        greets=(CORE,),
    )(a, b)


def placed(parts, pieces, last):
    shapes = [(8, 2, cut[-1][0].stop, cut[-1][1].stop) for cut in pieces]
    last = [one.reshape(shape) for one, shape in zip(last, shapes, strict=True)]

    def kernel(*refs):
        came, went = refs[-2:]
        me = lax.axis_index("dp")
        core, pair = me & 1, me >> 1

        def copies(which, j):
            held = refs[15 + which]
            bits = {"x": j >> 2, "y": (j >> 1) & 1, "z": j & 1}
            for i, (rows, cols, order) in enumerate(pieces[which]):
                at = bits[order[0]] * 4 + bits[order[1]] * 2 + bits[order[2]]
                for side in range(2):
                    src = refs[3 * which + i].at[8 * side + at]
                    dst = held.at[pair ^ j, core ^ side, rows, cols]
                    yield pltpu.make_async_copy(src, dst, came.at[which, j, 2 * i + side])

        def leave(which, j):
            k = pair ^ j
            return pltpu.make_async_copy(refs[15 + which].at[k], refs[12 + which].at[0, k], went.at[which, j])

        into = [pltpu.make_async_copy(refs[9 + k], refs[18 + k], came.at[k, 8, 0]) for k in range(3)]
        off = [pltpu.make_async_copy(refs[18 + k], refs[12 + k].at[1], went.at[k, 8]) for k in range(3)]
        for which in range(3):
            into[which].start()
        for which in range(3):
            for j in range(8):
                for copy in copies(which, j):
                    copy.start()
        for which in range(3):
            into[which].wait()
            off[which].start()
        for which in range(3):
            for j in range(8):
                for copy in copies(which, j):
                    copy.wait()
                leave(which, j).start()
        for which in range(3):
            off[which].wait()
            for j in range(8):
                leave(which, j).wait()

    whole = pl.BlockSpec(memory_space=pl.ANY)
    return list(
        pl.pallas_call(
            kernel,
            in_specs=[whole] * 12,
            out_specs=[whole] * 3,
            out_shape=like(*[((2, *shape), BF) for shape in shapes]),
            scratch_shapes=[
                *[pltpu.VMEM(shape, BF) for shape in shapes] * 2,
                pltpu.SemaphoreType.DMA((3, 9, 6)),
                pltpu.SemaphoreType.DMA((3, 9)),
            ],
            cost_estimate=pl.CostEstimate(flops=10**9, bytes_accessed=10**7, transcendentals=0),
            compiler_params=pltpu.CompilerParams(vmem_limit_bytes=VMEM),
            name="placed",
        )(*parts[0], *parts[1], *parts[2], *last)
    )


BITS = {"x": 4, "y": 2, "z": 1}


def peer(bit):
    return {"dp": lax.axis_index("dp") ^ bit}


def remote(src, dst, sems, i, bit):
    return pltpu.make_async_remote_copy(
        src, dst, sems[0].at[i], sems[1].at[i], device_id=peer(bit), device_id_type=pl.DeviceIdType.MESH
    )


def greet(bits):
    barrier = pltpu.get_barrier_semaphore()
    for bit in bits:
        pl.semaphore_signal(barrier, inc=1, device_id=peer(bit), device_id_type=pl.DeviceIdType.MESH)
    pl.semaphore_wait(barrier, len(bits))


class Summed:
    def __init__(self, pieces, refs):
        self.pieces = pieces
        self.mine, self.other = refs[:2]
        self.out = [refs[2 + 3 * i : 5 + 3 * i] for i in range(3)]
        self.got = [refs[11 + 3 * i : 14 + 3 * i] for i in range(3)]
        self.sems = refs[20:22]

    @staticmethod
    def scratch(pieces, shape):
        whole = [pltpu.VMEM((8, *shape), BF)] * 2
        halves = [pltpu.VMEM((n, size(rows), size(cols)), BF) for rows, cols, _ in pieces for n in (4, 2, 1)]
        return [*whole, *halves, *halves, pltpu.SemaphoreType.DMA((9,)), pltpu.SemaphoreType.DMA((9,))]

    def copy(self, i, stage):
        return remote(self.out[i][stage], self.got[i][stage], self.sems, 3 * i + stage, BIT[self.pieces[i][2][stage]])

    def term(self, i, stage, j):
        rows, cols, order = self.pieces[i]
        total = self.mine[j, rows, cols].astype(F32) + self.other[j, rows, cols].astype(F32)
        for past in range(stage):
            total = total + self.got[i][past][self.place(order, past, j)].astype(F32)
        return total

    @staticmethod
    def place(order, stage, j):
        rest = [axis for axis in "xyz" if axis not in order[: stage + 1]]
        return sum(bool(j & BITS[axis]) << (len(rest) - 1 - k) for k, axis in enumerate(rest))

    def send(self, stage, i):
        order = self.pieces[i][2]
        if stage:
            self.copy(i, stage - 1).wait_recv()
        for j in range(8):
            gone = any(j & BITS[axis] for axis in order[:stage])
            if j & BITS[order[stage]] and not gone:
                self.out[i][stage][self.place(order, stage, j)] = self.term(i, stage, j).astype(BF)
        self.copy(i, stage).start()

    def total(self, i):
        self.copy(i, 2).wait_recv()
        return self.term(i, 3, 0).astype(BF).astype(F32)

    def finish(self):
        for i in range(3):
            for stage in range(3):
                self.copy(i, stage).wait_send()


class Sum:
    def __init__(self, pieces, keep, got, plan=()):
        self.pieces, self.arrays = pieces, [keep, got]
        self.shape = keep.shape[1:]
        self.plan = [(0, "load"), *[(at, (stage, i)) for stage, at in enumerate(plan) for i in range(3)]]

    def results(self):
        return [(pl.BlockSpec(self.shape, lambda i: (0, 0)), jax.ShapeDtypeStruct(self.shape, BF))]

    def scratch(self):
        return [*Summed.scratch(self.pieces, self.shape), pltpu.SemaphoreType.DMA((2,))]

    def bind(self, ins, outs, refs):
        one = Sum.__new__(Sum)
        one.pieces, one.given = self.pieces, ins
        one.out = outs[0] if outs else None
        one.sum, one.local = Summed(self.pieces, refs[:22]), refs[22]
        return one

    def copies(self):
        into = (self.sum.mine, self.sum.other)
        return [pltpu.make_async_copy(self.given[k], into[k], self.local.at[k]) for k in range(2)]

    def run(self, part):
        if part == "load":
            for copy in self.copies():
                copy.start()
            return
        stage, i = part
        if part == (0, 0):
            for copy in self.copies():
                copy.wait()
        self.sum.send(stage, i)

    def end(self):
        for i, (rows, cols, _) in enumerate(self.pieces):
            self.out[rows, cols] = self.sum.total(i).astype(BF)
        self.sum.finish()


class Spread:
    def __init__(self, pieces, block, plan=()):
        self.pieces, self.arrays, self.shape = pieces, [block], block.shape
        self.plan = list(zip(plan, ("begin", 0, 1, 2)))

    def results(self):
        return [
            (pl.BlockSpec(memory_space=pl.ANY), jax.ShapeDtypeStruct((16, size(rows), size(cols)), BF))
            for rows, cols, _ in self.pieces
        ]

    @staticmethod
    def scratch():
        return [pltpu.SemaphoreType.DMA((27,)), pltpu.SemaphoreType.DMA((27,)), pltpu.SemaphoreType.DMA((3,))]

    def bind(self, ins, outs, sems):
        own = ins if len(ins) == 3 else [ins[0].at[rows, cols] for rows, cols, _ in self.pieces]
        one = Spread.__new__(Spread)
        one.pieces, one.own, one.outs = self.pieces, own, outs
        one.sems, one.local = sems[:2], sems[2]
        return one

    def along(self, i, stage):
        out, n, bit = self.outs[i], 1 << stage, BIT[self.pieces[i][2][2 - stage]]
        copies = [remote(self.own[i], out.at[n], self.sems, 9 * i + 2 * stage, bit)]
        if stage:
            src, dst = out.at[pl.ds(1, n - 1)], out.at[pl.ds(n + 1, n - 1)]
            copies.append(remote(src, dst, self.sems, 9 * i + 2 * stage - 1, bit))
        return copies

    def across(self, i, stage):
        out, at = self.outs[i], 9 * i + 5 + stage
        if stage == 0:
            return remote(self.own[i], out.at[8], self.sems, at, CORE)
        n = 1 << (stage - 1)
        return remote(out.at[pl.ds(n, n)], out.at[pl.ds(8 + n, n)], self.sems, at, CORE)

    def keep(self, i):
        return pltpu.make_async_copy(self.own[i], self.outs[i].at[0], self.local.at[i])

    def begin(self, i):
        for copy in self.along(i, 0):
            copy.start()
        self.across(i, 0).start()
        self.keep(i).start()

    def step(self, stage, i):
        for copy in self.along(i, stage):
            copy.wait_recv()
        if stage < 2:
            for copy in self.along(i, stage + 1):
                copy.start()
        self.across(i, stage + 1).start()

    def run(self, part):
        for i in range(3):
            self.begin(i) if part == "begin" else self.step(part, i)

    def end(self):
        for i in range(3):
            self.keep(i).wait()
            for stage in range(3):
                for copy in self.along(i, stage):
                    copy.wait_send()
            for stage in range(4):
                self.across(i, stage).wait()


def tail(gate, up, states, pieces):
    rows, width = gate[0].shape[1:]

    both = [Sum(pieces[k], *(gate, up)[k]) for k in range(2)]
    ways = [Spread(pieces[k], jax.ShapeDtypeStruct((rows, width), BF)) for k in range(2)]

    def kernel(*refs):
        w_in, m_in, v_in = ((refs[4 + k], refs[7 + k]) for k in range(3))
        outs = [refs[10 + 3 * k : 13 + 3 * k] for k in range(2)]
        m_out, v_out = refs[16:18], refs[18:20]
        sums = [both[k].bind(refs[2 * k : 2 * k + 2], None, refs[20 + 23 * k : 43 + 23 * k]) for k in range(2)]
        own = [refs[66:69], refs[69:72]]
        spread = [ways[k].bind(own[k], outs[k], refs[72 + 3 * k : 75 + 3 * k]) for k in range(2)]
        greet(ALL)
        for one in sums:
            one.run("load")
        for stage in range(3):
            for one in sums:
                for i in range(3):
                    one.run((stage, i))
        for k in range(2):
            for i, (_, cols, _) in enumerate(pieces[k]):
                new, m_out[k][:, cols], v_out[k][:, cols] = adamw(
                    w_in[k][:, cols].astype(F32), m_in[k][:, cols], v_in[k][:, cols], sums[k].sum.total(i)
                )
                own[k][i][...] = new
                spread[k].begin(i)
        for stage in range(3):
            for k in range(2):
                spread[k].run(stage)
        for k in range(2):
            sums[k].sum.finish()
            spread[k].end()

    hbm, vmem = pl.BlockSpec(memory_space=pl.ANY), pl.BlockSpec(memory_space=pltpu.VMEM)
    arrays = [jax.ShapeDtypeStruct((16, rows, size(cols)), BF) for k in range(2) for _, cols, _ in pieces[k]]
    state = [jax.ShapeDtypeStruct((rows, width), F32)] * 4
    out = pl.pallas_call(
        kernel,
        in_specs=[hbm] * 4 + [vmem] * 6,
        out_specs=[hbm] * 6 + [vmem] * 4,
        out_shape=[*arrays, *state],
        scratch_shapes=[
            *both[0].scratch(),
            *both[1].scratch(),
            *[pltpu.VMEM((rows, size(cols)), BF) for k in range(2) for _, cols, _ in pieces[k]],
            *Spread.scratch() * 2,
        ],
        cost_estimate=pl.CostEstimate(flops=10**11, bytes_accessed=10**8, transcendentals=0),
        compiler_params=pltpu.CompilerParams(collective_id=1, has_side_effects=True, vmem_limit_bytes=VMEM),
        name="tail",
    )(*gate, *up, *states[0], *states[1])
    return [out[3 * k : 3 * k + 3] for k in range(2)], out[6:8], out[8:10]


def adamw(w, m, v, g):
    m = 0.9 * m + 0.1 * g
    v = 0.95 * v + 0.05 * g * g
    step = m * lax.rsqrt(v + 1e-8) + 0.1 * w
    return (w - 0.02 * step).astype(BF), m, v


def solution(mesh):
    ORDERS = ("xyz", "yzx", "zxy")

    def body(x, dy, w_gate, w_up, w_down, *moments):
        x, dy = x[0], dy[0]
        m, v = moments[:3], moments[3:]
        me = lax.axis_index("dp")
        weights = (w_gate, w_up, w_down)
        new = [[None] * 2 for _ in range(9)]

        def pieces_of(which):
            orders = [ORDERS[(which + i) % 3] for i in range(3)]
            rows, width = weights[which].shape[1] // 16, weights[which].shape[2]
            if which == 2:
                ends = [0, 80, 160, rows]
                return [(slice(ends[i], ends[i + 1]), slice(0, width), orders[i]) for i in range(3)]
            ends = [0, 1152, 2304, width]
            return [(slice(0, rows), slice(ends[i], ends[i + 1]), orders[i]) for i in range(3)]

        def state(which, n):
            rows, width = weights[which].shape[1] // 16, weights[which].shape[2]
            w = lax.dynamic_slice(weights[which], (n, me * rows, 0), (1, rows, width))[0]
            return w, m[which][n], v[which][n]

        def update(which, n, g):
            w, m1, v1 = state(which, n)
            w, new[3 + which][n], new[6 + which][n] = adamw(w.astype(F32), m1, v1, g.astype(F32))
            return w

        def everywhere(w):
            return lax.all_gather(w, "dp", axis=0, tiled=True)

        a0 = normed(x)
        gate, up, hid0 = forward(a0, w_gate, w_up, 0)
        h, a1 = down(x, hid0, w_down, 0)
        hid1, d_gate, d_up = turn(a1, dy, w_gate, w_up, w_down, 1)
        pieces = [pieces_of(which) for which in range(3)]
        down1 = by_rows(hid1, dy, 5)
        sides = [Sum(pieces[2], *down1, (1, 7, 10))]
        *both, g = by_columns(a1, (d_gate, d_up), sides=sides, collective_id=2)
        w_d1 = everywhere(update(2, 1, g))
        sides = [
            Sum(pieces[0], *both[::2], (0, 3, 6)),
            Sum(pieces[1], *both[1::2], (1, 5, 7)),
        ]
        back, g_g1, g_u1 = through(d_gate, d_up, w_gate, w_up, h, dy, 1, sides=sides, collective_id=3)
        w_g1, w_u1 = everywhere(update(0, 1, g_g1)), everywhere(update(1, 1, g_u1))
        sides = [Sum(pieces[2], *by_rows(hid0, back, 7), (1, 6, 9))]
        d_gate, d_up, g = backward(back, gate, up, w_down, 0, sides=sides, collective_id=4)
        sides = [Spread(pieces[2], update(2, 0, g), (0, 3, 7, 13))]
        *both, p0, p1, p2 = by_columns(a0, (d_gate, d_up), sides=sides, collective_id=6)
        parts, ms, vs = tail(both[::2], both[1::2], (state(0, 0), state(1, 0)), pieces)
        for which in range(2):
            new[3 + which][0], new[6 + which][0] = ms[which], vs[which]
        whole = placed([*parts, (p0, p1, p2)], pieces, (w_g1, w_u1, w_d1))
        for i in range(3):
            new[i] = whole[i].reshape(weights[i].shape)
        return tuple(one if i < 3 else jnp.stack(one) for i, one in enumerate(new))

    seq = P(("rep", "dp"), None, None)
    full = P(None, None, None)
    block = P(None, "dp", None)
    return jax.shard_map(
        body,
        mesh=mesh,
        in_specs=(seq, seq, *[full] * 3, *[block] * 6),
        out_specs=(*[P("rep", None, None)] * 3, *[P("rep", "dp", None)] * 6),
        check_vma=False,
    )
```

```python
import jax
import jax.numpy as jnp
from jax import lax
from jax.experimental import pallas as pl
from jax.experimental.pallas import tpu as pltpu
from jax.sharding import PartitionSpec as P

BF, F32 = jnp.bfloat16, jnp.float32
CORE = 1
BIT = {"x": 8, "y": 4, "z": 2}
ALL = (CORE, *BIT.values())
VMEM = 60 * 2**20


def dot(a, b, ca, cb):
    return lax.dot_general(a, b, (((ca,), (cb,)), ((), ())), preferred_element_type=F32)


def call(kernel, grid, ins, outs, shapes, flops, scratch=(), aliases={}, sides=(), collective_id=None, greets=()):
    several = isinstance(shapes, list)
    outs, shapes = (outs, shapes) if several else ([outs], [shapes])
    n_in, n_out, n_scratch = len(ins), len(outs), len(scratch)
    hbm = pl.BlockSpec(memory_space=pl.ANY)
    arrays = [array for side in sides for array in side.arrays]
    results = [one for side in sides for one in side.results()]
    more = [side.scratch() for side in sides]

    def whole(*refs):
        take = iter(refs)

        def some(n):
            return [next(take) for _ in range(n)]

        main = some(n_in)
        given = [some(len(side.arrays)) for side in sides]
        main += some(n_out)
        made = [some(len(side.results())) for side in sides]
        main += some(n_scratch)
        running = [
            side.bind(given[k], made[k], some(len(more[k]))) for k, side in enumerate(sides)
        ]
        step = pl.program_id(0)
        if greets:

            @pl.when(step == 0)
            def _():
                greet(greets)

        for at in sorted({at for side in sides for at, _ in side.plan}):

            @pl.when(step == at)
            def _():
                for side, one in zip(sides, running, strict=True):
                    for when, part in side.plan:
                        if when == at:
                            one.run(part)

        kernel(*main)
        if sides:

            @pl.when(step == grid[0] - 1)
            def _():
                for one in running:
                    one.end()

    out = pl.pallas_call(
        whole,
        grid=grid,
        in_specs=[*ins, *[hbm] * len(arrays)],
        out_specs=[*outs, *[spec for spec, _ in results]],
        out_shape=[*shapes, *[shape for _, shape in results]],
        scratch_shapes=[*scratch, *[one for group in more for one in group]],
        input_output_aliases=aliases,
        cost_estimate=pl.CostEstimate(flops=flops, bytes_accessed=flops // 400, transcendentals=0),
        compiler_params=pltpu.CompilerParams(
            vmem_limit_bytes=VMEM,
            dimension_semantics=("arbitrary",) * len(grid),
            collective_id=collective_id,
            has_side_effects=bool(greets),
        ),
    )

    def run(*args):
        got = out(*args, *arrays)
        return got if several or sides else got[0]

    return run


def size(part):
    return part.stop - part.start


def like(*shapes):
    return [jax.ShapeDtypeStruct(s, d) for s, d in shapes]


def scale_of(wide):
    return lax.rsqrt(jnp.mean(wide**2, -1, keepdims=True) + 1e-6)


def normed(h):
    wide = h.astype(F32)
    return (wide * scale_of(wide)).astype(BF)


def forward(a, w_gate, w_up, n, tile=256):
    t, d = a.shape
    ff = w_gate.shape[2]

    def kernel(a, wg, wu, gate, up, hid):
        for r in range(0, t, 512):
            r = slice(r, r + 512)
            g = dot(a[r], wg[...], 1, 0)
            u = dot(a[r], wu[...], 1, 0)
            gate[r] = g
            up[r] = u
            hid[r] = (g * sigmoid(g) * u).astype(BF)

    w = pl.BlockSpec((None, d, tile), lambda j: (n, 0, j))
    o = pl.BlockSpec((t, tile), lambda j: (0, j))
    return call(
        kernel,
        (ff // tile,),
        [pl.BlockSpec((t, d), lambda j: (0, 0)), w, w],
        [o, o, o],
        like(((t, ff), F32), ((t, ff), F32), ((t, ff), BF)),
        4 * t * d * ff,
    )(a, w_gate, w_up)


def down(x, hid, w_down, n, tile=512):
    t, d = x.shape
    ff = hid.shape[1]

    def kernel(x, hid, w, h, a):
        new = x[...].astype(F32) + dot(hid[...], w[...], 1, 0).astype(BF).astype(F32)
        new = new.astype(BF)
        h[...] = new
        a[...] = normed(new)

    o = pl.BlockSpec((tile, d), lambda i: (i, 0))
    return call(
        kernel,
        (t // tile,),
        [o, pl.BlockSpec((tile, ff), lambda i: (i, 0)), pl.BlockSpec((None, ff, d), lambda i: (n, 0, 0))],
        [o, o],
        like(((t, d), BF), ((t, d), BF)),
        2 * t * d * ff,
    )(x, hid, w_down)


def sigmoid(x):
    return 0.5 * jnp.tanh(0.5 * x) + 0.5


def gated_back(g, u, d_hid):
    d_hid = d_hid.astype(BF).astype(F32)
    s = sigmoid(g)
    act = g * s
    d_up = (d_hid * act).astype(BF)
    d_gate = (d_hid * u * (s + act * (1 - s))).astype(BF)
    return act, d_gate, d_up


def turn(a, back, w_gate, w_up, w_down, n, tile=256):
    t, d = a.shape
    ff = w_gate.shape[2]

    def kernel(a, back, wg, wu, wd, hid, d_gate, d_up):
        for r in range(0, t, 512):
            r = slice(r, r + 512)
            g = dot(a[r], wg[...], 1, 0)
            u = dot(a[r], wu[...], 1, 0)
            act, d_gate[r], d_up[r] = gated_back(g, u, dot(back[r], wd[...], 1, 1))
            hid[r] = (act * u).astype(BF)

    whole = pl.BlockSpec((t, d), lambda j: (0, 0))
    w = pl.BlockSpec((None, d, tile), lambda j: (n, 0, j))
    o = pl.BlockSpec((t, tile), lambda j: (0, j))
    return call(
        kernel,
        (ff // tile,),
        [whole, whole, w, w, pl.BlockSpec((None, tile, d), lambda j: (n, j, 0))],
        [o, o, o],
        like(*[((t, ff), BF)] * 3),
        6 * t * d * ff,
    )(a, back, w_gate, w_up, w_down)


def backward(back, gate, up, w_down, n, tile=256, sides=(), collective_id=None):
    t, d = back.shape
    ff = gate.shape[1]

    def kernel(back, wd, g, u, d_gate, d_up):
        for r in range(0, t, 512):
            r = slice(r, r + 512)
            _, d_gate[r], d_up[r] = gated_back(g[r], u[r], dot(back[r], wd[...], 1, 1))

    o = pl.BlockSpec((t, tile), lambda j: (0, j))
    return call(
        kernel,
        (ff // tile,),
        [once((t, d), lambda j: (0, 0)), pl.BlockSpec((None, tile, d), lambda j: (n, j, 0)), o, o],
        [o, o],
        like(*[((t, ff), BF)] * 2),
        2 * t * d * ff,
        sides=sides,
        greets=ALL,
        collective_id=collective_id,
    )(back, w_down, gate, up)


def through(d_gate, d_up, w_gate, w_up, h, back, n, tile=256, sides=(), collective_id=None):
    t, d = h.shape
    ff = d_gate.shape[1]

    def kernel(dg, du, wg, wu, h, back, out):
        d_a = dot(dg[...], wg[...], 1, 1).astype(BF).astype(F32) + dot(du[...], wu[...], 1, 1).astype(BF).astype(F32)
        d_a = d_a.astype(BF).astype(F32)
        wide = h[...].astype(F32)
        scale = scale_of(wide)
        along = jnp.mean(d_a * wide, -1, keepdims=True)
        d_h = scale * d_a - wide * (scale**3 * along)
        out[...] = (back[...].astype(F32) + d_h.astype(BF).astype(F32)).astype(BF)

    o = pl.BlockSpec((tile, d), lambda i: (i, 0))
    wide = pl.BlockSpec((tile, ff), lambda i: (i, 0))
    w = once((None, d, ff), lambda i: (n, 0, 0))
    return call(
        kernel,
        (t // tile,),
        [wide, wide, w, w, o, o],
        o,
        like(((t, d), BF))[0],
        4 * t * d * ff,
        sides=sides,
        greets=ALL,
        collective_id=collective_id,
    )(d_gate, d_up, w_gate, w_up, h, back)


def once(shape, index):
    return pl.BlockSpec(shape, index, pipeline_mode=pl.Buffered(1))


class Crossing:
    def __init__(self, steps, slots, sent, came):
        self.steps, self.slots, self.sems = steps, slots, (sent, came)

    @staticmethod
    def scratch(steps, shape):
        sems = pltpu.SemaphoreType.DMA((steps,))
        return [pltpu.VMEM((2, *shape), BF), sems, sems]

    def copy(self, at, dst):
        return remote(self.slots.at[at % 2], dst, self.sems, at, CORE)

    def slot(self, step, dst):
        @pl.when(step >= 2)
        def _():
            self.copy(step - 2, dst).wait_send()

        return self.slots.at[step % 2]

    def end(self, step, dst):
        @pl.when(step == self.steps - 1)
        def _():
            for at in range(self.steps):
                if at >= self.steps - 2:
                    self.copy(at, dst).wait_send()
                self.copy(at, dst).wait_recv()


def by_columns(a, bs, tile=512, sides=(), collective_id=None):
    t, d = a.shape
    ff = bs[0].shape[1]
    rows, steps = d // 16, ff // tile
    total = steps * len(bs)

    def kernel(a, *refs):
        ins, refs = refs[: len(bs)], refs[len(bs) :]
        kept, got, (acc, *rest) = refs[: len(bs)], refs[len(bs) : 2 * len(bs)], refs[2 * len(bs) :]
        crossing = Crossing(total, *rest)
        me, step = lax.axis_index("dp"), pl.program_id(0)
        slot = crossing.slot(step, got[0].at[:, :, pl.ds(0, tile)])
        for k in range(len(bs)):

            @pl.when(step // steps == k)
            def _():
                acc[...] = dot(a[...], ins[k][...], 0, 0).reshape(acc.shape)
                for j in range(8):
                    slot[j] = acc[(2 * j + 1) ^ me].astype(BF)
                for j in range(8):
                    kept[k][j] = acc[(2 * j) ^ me].astype(BF)
                cols = pl.ds(pl.multiple_of((step - k * steps) * tile, tile), tile)
                crossing.copy(step, got[k].at[:, :, cols]).start()

        crossing.end(step, got[0].at[:, :, pl.ds(0, tile)])

    def at(k):
        return lambda i: jnp.clip(i - k * steps, 0, steps - 1)

    ins = [pl.BlockSpec((t, tile), lambda i, k=k: (0, at(k)(i))) for k in range(len(bs))]
    outs = [pl.BlockSpec((8, rows, tile), lambda i, k=k: (0, 0, at(k)(i))) for k in range(len(bs))]
    return call(
        kernel,
        (total,),
        [once((t, d), lambda i: (0, 0)), *ins],
        [*outs, *[pl.BlockSpec(memory_space=pl.ANY)] * len(bs)],
        like(*[((8, rows, ff), BF)] * (2 * len(bs))),
        2 * t * d * ff * len(bs),
        scratch=[pltpu.VMEM((16, rows, tile), F32), *Crossing.scratch(total, (8, rows, tile))],
        sides=sides,
        collective_id=collective_id,
        greets=ALL,
    )(a, *bs)


def by_rows(a, b, collective_id):
    t, ff = a.shape
    d = b.shape[1]
    rows = ff // 16

    def kernel(a, b, keep, got, acc, *rest):
        crossing = Crossing(4, *rest)
        me, step = lax.axis_index("dp"), pl.program_id(0)
        slot = crossing.slot(step, got.at[pl.ds(0, 2)])
        acc[...] = dot(a[...], b[...], 0, 0).reshape(acc.shape)
        low = me & 3
        for j in range(2):
            slot[j] = acc[(2 * j + 1) ^ low].astype(BF)
        for j in range(2):
            keep[j] = acc[(2 * j) ^ low].astype(BF)
        crossing.copy(step, got.at[pl.ds(2 * (step ^ (me >> 2)), 2)]).start()
        crossing.end(step, got.at[pl.ds(0, 2)])

    return call(
        kernel,
        (4,),
        [pl.BlockSpec((t, ff // 4), lambda i: (0, i)), once((t, d), lambda i: (0, 0))],
        [pl.BlockSpec((2, rows, d), lambda i: (i ^ (lax.axis_index("dp") >> 2), 0, 0)), pl.BlockSpec(memory_space=pl.ANY)],
        like(*[((8, rows, d), BF)] * 2),
        2 * t * d * ff,
        scratch=[pltpu.VMEM((4, rows, d), F32), *Crossing.scratch(4, (2, rows, d))],
        collective_id=collective_id,
        greets=(CORE,),
    )(a, b)


def placed(parts, pieces, last):
    shapes = [(8, 2, cut[-1][0].stop, cut[-1][1].stop) for cut in pieces]
    last = [one.reshape(shape) for one, shape in zip(last, shapes, strict=True)]

    def kernel(*refs):
        came, went = refs[-2:]
        me = lax.axis_index("dp")
        core, pair = me & 1, me >> 1

        def copies(which, j):
            held = refs[15 + which]
            bits = {"x": j >> 2, "y": (j >> 1) & 1, "z": j & 1}
            for i, (rows, cols, order) in enumerate(pieces[which]):
                at = bits[order[0]] * 4 + bits[order[1]] * 2 + bits[order[2]]
                for side in range(2):
                    src = refs[3 * which + i].at[8 * side + at]
                    dst = held.at[pair ^ j, core ^ side, rows, cols]
                    yield pltpu.make_async_copy(src, dst, came.at[which, j, 2 * i + side])

        def leave(which, j):
            k = pair ^ j
            return pltpu.make_async_copy(refs[15 + which].at[k], refs[12 + which].at[0, k], went.at[which, j])

        into = [pltpu.make_async_copy(refs[9 + k], refs[18 + k], came.at[k, 8, 0]) for k in range(3)]
        off = [pltpu.make_async_copy(refs[18 + k], refs[12 + k].at[1], went.at[k, 8]) for k in range(3)]
        for which in range(3):
            into[which].start()
        for which in range(3):
            for j in range(8):
                for copy in copies(which, j):
                    copy.start()
        for which in range(3):
            into[which].wait()
            off[which].start()
        for which in range(3):
            for j in range(8):
                for copy in copies(which, j):
                    copy.wait()
                leave(which, j).start()
        for which in range(3):
            off[which].wait()
            for j in range(8):
                leave(which, j).wait()

    whole = pl.BlockSpec(memory_space=pl.ANY)
    return list(
        pl.pallas_call(
            kernel,
            in_specs=[whole] * 12,
            out_specs=[whole] * 3,
            out_shape=like(*[((2, *shape), BF) for shape in shapes]),
            scratch_shapes=[
                *[pltpu.VMEM(shape, BF) for shape in shapes] * 2,
                pltpu.SemaphoreType.DMA((3, 9, 6)),
                pltpu.SemaphoreType.DMA((3, 9)),
            ],
            cost_estimate=pl.CostEstimate(flops=10**9, bytes_accessed=10**7, transcendentals=0),
            compiler_params=pltpu.CompilerParams(vmem_limit_bytes=VMEM),
            name="placed",
        )(*parts[0], *parts[1], *parts[2], *last)
    )


BITS = {"x": 4, "y": 2, "z": 1}


def peer(bit):
    return {"dp": lax.axis_index("dp") ^ bit}


def remote(src, dst, sems, i, bit):
    return pltpu.make_async_remote_copy(
        src, dst, sems[0].at[i], sems[1].at[i], device_id=peer(bit), device_id_type=pl.DeviceIdType.MESH
    )


def greet(bits):
    barrier = pltpu.get_barrier_semaphore()
    for bit in bits:
        pl.semaphore_signal(barrier, inc=1, device_id=peer(bit), device_id_type=pl.DeviceIdType.MESH)
    pl.semaphore_wait(barrier, len(bits))


class Summed:
    def __init__(self, pieces, refs):
        self.pieces = pieces
        self.mine, self.other = refs[:2]
        self.out = [refs[2 + 3 * i : 5 + 3 * i] for i in range(3)]
        self.got = [refs[11 + 3 * i : 14 + 3 * i] for i in range(3)]
        self.sems = refs[20:22]

    @staticmethod
    def scratch(pieces, shape):
        whole = [pltpu.VMEM((8, *shape), BF)] * 2
        halves = [pltpu.VMEM((n, size(rows), size(cols)), BF) for rows, cols, _ in pieces for n in (4, 2, 1)]
        return [*whole, *halves, *halves, pltpu.SemaphoreType.DMA((9,)), pltpu.SemaphoreType.DMA((9,))]

    def copy(self, i, stage):
        return remote(self.out[i][stage], self.got[i][stage], self.sems, 3 * i + stage, BIT[self.pieces[i][2][stage]])

    def term(self, i, stage, j):
        rows, cols, order = self.pieces[i]
        total = self.mine[j, rows, cols].astype(F32) + self.other[j, rows, cols].astype(F32)
        for past in range(stage):
            total = total + self.got[i][past][self.place(order, past, j)].astype(F32)
        return total

    @staticmethod
    def place(order, stage, j):
        rest = [axis for axis in "xyz" if axis not in order[: stage + 1]]
        return sum(bool(j & BITS[axis]) << (len(rest) - 1 - k) for k, axis in enumerate(rest))

    def send(self, stage, i):
        order = self.pieces[i][2]
        if stage:
            self.copy(i, stage - 1).wait_recv()
        for j in range(8):
            gone = any(j & BITS[axis] for axis in order[:stage])
            if j & BITS[order[stage]] and not gone:
                self.out[i][stage][self.place(order, stage, j)] = self.term(i, stage, j).astype(BF)
        self.copy(i, stage).start()

    def total(self, i):
        self.copy(i, 2).wait_recv()
        return self.term(i, 3, 0).astype(BF).astype(F32)

    def finish(self):
        for i in range(3):
            for stage in range(3):
                self.copy(i, stage).wait_send()


class Sum:
    def __init__(self, pieces, keep, got, plan=()):
        self.pieces, self.arrays = pieces, [keep, got]
        self.shape = keep.shape[1:]
        self.plan = [(0, "load"), *[(at, (stage, i)) for stage, at in enumerate(plan) for i in range(3)]]

    def results(self):
        return [(pl.BlockSpec(self.shape, lambda i: (0, 0)), jax.ShapeDtypeStruct(self.shape, BF))]

    def scratch(self):
        return [*Summed.scratch(self.pieces, self.shape), pltpu.SemaphoreType.DMA((2,))]

    def bind(self, ins, outs, refs):
        one = Sum.__new__(Sum)
        one.pieces, one.given = self.pieces, ins
        one.out = outs[0] if outs else None
        one.sum, one.local = Summed(self.pieces, refs[:22]), refs[22]
        return one

    def copies(self):
        into = (self.sum.mine, self.sum.other)
        return [pltpu.make_async_copy(self.given[k], into[k], self.local.at[k]) for k in range(2)]

    def run(self, part):
        if part == "load":
            for copy in self.copies():
                copy.start()
            return
        stage, i = part
        if part == (0, 0):
            for copy in self.copies():
                copy.wait()
        self.sum.send(stage, i)

    def end(self):
        for i, (rows, cols, _) in enumerate(self.pieces):
            self.out[rows, cols] = self.sum.total(i).astype(BF)
        self.sum.finish()


class Spread:
    def __init__(self, pieces, block, plan=()):
        self.pieces, self.arrays, self.shape = pieces, [block], block.shape
        self.plan = list(zip(plan, ("begin", 0, 1, 2)))

    def results(self):
        return [
            (pl.BlockSpec(memory_space=pl.ANY), jax.ShapeDtypeStruct((16, size(rows), size(cols)), BF))
            for rows, cols, _ in self.pieces
        ]

    @staticmethod
    def scratch():
        return [pltpu.SemaphoreType.DMA((27,)), pltpu.SemaphoreType.DMA((27,)), pltpu.SemaphoreType.DMA((3,))]

    def bind(self, ins, outs, sems):
        own = ins if len(ins) == 3 else [ins[0].at[rows, cols] for rows, cols, _ in self.pieces]
        one = Spread.__new__(Spread)
        one.pieces, one.own, one.outs = self.pieces, own, outs
        one.sems, one.local = sems[:2], sems[2]
        return one

    def along(self, i, stage):
        out, n, bit = self.outs[i], 1 << stage, BIT[self.pieces[i][2][2 - stage]]
        copies = [remote(self.own[i], out.at[n], self.sems, 9 * i + 2 * stage, bit)]
        if stage:
            src, dst = out.at[pl.ds(1, n - 1)], out.at[pl.ds(n + 1, n - 1)]
            copies.append(remote(src, dst, self.sems, 9 * i + 2 * stage - 1, bit))
        return copies

    def across(self, i, stage):
        out, at = self.outs[i], 9 * i + 5 + stage
        if stage == 0:
            return remote(self.own[i], out.at[8], self.sems, at, CORE)
        n = 1 << (stage - 1)
        return remote(out.at[pl.ds(n, n)], out.at[pl.ds(8 + n, n)], self.sems, at, CORE)

    def keep(self, i):
        return pltpu.make_async_copy(self.own[i], self.outs[i].at[0], self.local.at[i])

    def begin(self, i):
        for copy in self.along(i, 0):
            copy.start()
        self.across(i, 0).start()
        self.keep(i).start()

    def step(self, stage, i):
        for copy in self.along(i, stage):
            copy.wait_recv()
        if stage < 2:
            for copy in self.along(i, stage + 1):
                copy.start()
        self.across(i, stage + 1).start()

    def run(self, part):
        for i in range(3):
            self.begin(i) if part == "begin" else self.step(part, i)

    def end(self):
        for i in range(3):
            self.keep(i).wait()
            for stage in range(3):
                for copy in self.along(i, stage):
                    copy.wait_send()
            for stage in range(4):
                self.across(i, stage).wait()


def tail(gate, up, states, pieces):
    rows, width = gate[0].shape[1:]

    both = [Sum(pieces[k], *(gate, up)[k]) for k in range(2)]
    ways = [Spread(pieces[k], jax.ShapeDtypeStruct((rows, width), BF)) for k in range(2)]

    def kernel(*refs):
        w_in, m_in, v_in = (refs[4 + 2 * k : 6 + 2 * k] for k in range(3))
        outs = [refs[10 + 3 * k : 13 + 3 * k] for k in range(2)]
        m_out, v_out = refs[16:18], refs[18:20]
        sums = [both[k].bind(refs[2 * k : 2 * k + 2], None, refs[20 + 23 * k : 43 + 23 * k]) for k in range(2)]
        own = [refs[66:69], refs[69:72]]
        spread = [ways[k].bind(own[k], outs[k], refs[72 + 3 * k : 75 + 3 * k]) for k in range(2)]
        greet(ALL)
        for one in sums:
            one.run("load")
        for stage in range(3):
            for one in sums:
                for i in range(3):
                    one.run((stage, i))
        for k in range(2):
            for i, (_, cols, _) in enumerate(pieces[k]):
                new, m_out[k][:, cols], v_out[k][:, cols] = adamw(
                    w_in[k][:, cols].astype(F32), m_in[k][:, cols], v_in[k][:, cols], sums[k].sum.total(i)
                )
                own[k][i][...] = new
                spread[k].begin(i)
        for stage in range(3):
            for k in range(2):
                spread[k].run(stage)
        for k in range(2):
            sums[k].sum.finish()
            spread[k].end()

    hbm, vmem = pl.BlockSpec(memory_space=pl.ANY), once((rows, width), lambda i: (0, 0))
    first = once((None, rows, width), lambda i: (0, 0, 0))
    mine = once((None, rows, width), lambda i: (0, lax.axis_index("dp"), 0))
    arrays = [jax.ShapeDtypeStruct((16, rows, size(cols)), BF) for k in range(2) for _, cols, _ in pieces[k]]
    state = [jax.ShapeDtypeStruct((rows, width), F32)] * 4
    out = pl.pallas_call(
        kernel,
        grid=(1,),
        in_specs=[hbm] * 4 + [mine] * 2 + [first] * 4,
        out_specs=[hbm] * 6 + [vmem] * 4,
        out_shape=[*arrays, *state],
        scratch_shapes=[
            *both[0].scratch(),
            *both[1].scratch(),
            *[pltpu.VMEM((rows, size(cols)), BF) for k in range(2) for _, cols, _ in pieces[k]],
            *Spread.scratch() * 2,
        ],
        cost_estimate=pl.CostEstimate(flops=10**11, bytes_accessed=10**8, transcendentals=0),
        compiler_params=pltpu.CompilerParams(collective_id=1, has_side_effects=True, vmem_limit_bytes=VMEM),
        name="tail",
    )(*gate, *up, *[state[i] for i in range(3) for state in states])
    return [out[3 * k : 3 * k + 3] for k in range(2)], out[6:8], out[8:10]


def adamw(w, m, v, g):
    m = 0.9 * m + 0.1 * g
    v = 0.95 * v + 0.05 * g * g
    step = m * lax.rsqrt(v + 1e-8) + 0.1 * w
    return (w - 0.02 * step).astype(BF), m, v


def solution(mesh):
    ORDERS = ("xyz", "yzx", "zxy")

    def body(x, dy, w_gate, w_up, w_down, *moments):
        x, dy = x[0], dy[0]
        m, v = moments[:3], moments[3:]
        me = lax.axis_index("dp")
        weights = (w_gate, w_up, w_down)
        new = [[None] * 2 for _ in range(9)]

        def pieces_of(which):
            orders = [ORDERS[(which + i) % 3] for i in range(3)]
            rows, width = weights[which].shape[1] // 16, weights[which].shape[2]
            if which == 2:
                ends = [0, 80, 160, rows]
                return [(slice(ends[i], ends[i + 1]), slice(0, width), orders[i]) for i in range(3)]
            ends = [0, 1152, 2304, width]
            return [(slice(0, rows), slice(ends[i], ends[i + 1]), orders[i]) for i in range(3)]

        def state(which, n):
            rows, width = weights[which].shape[1] // 16, weights[which].shape[2]
            w = lax.dynamic_slice(weights[which], (n, me * rows, 0), (1, rows, width))[0]
            return w, m[which][n], v[which][n]

        def update(which, n, g):
            w, m1, v1 = state(which, n)
            w, new[3 + which][n], new[6 + which][n] = adamw(w.astype(F32), m1, v1, g.astype(F32))
            return w

        def everywhere(w):
            return lax.all_gather(w, "dp", axis=0, tiled=True)

        a0 = normed(x)
        gate, up, hid0 = forward(a0, w_gate, w_up, 0)
        h, a1 = down(x, hid0, w_down, 0)
        hid1, d_gate, d_up = turn(a1, dy, w_gate, w_up, w_down, 1)
        pieces = [pieces_of(which) for which in range(3)]
        down1 = by_rows(hid1, dy, 5)
        sides = [Sum(pieces[2], *down1, (1, 7, 10))]
        *both, g = by_columns(a1, (d_gate, d_up), sides=sides, collective_id=2)
        w_d1 = everywhere(update(2, 1, g))
        sides = [
            Sum(pieces[0], *both[::2], (0, 3, 6)),
            Sum(pieces[1], *both[1::2], (1, 5, 7)),
        ]
        back, g_g1, g_u1 = through(d_gate, d_up, w_gate, w_up, h, dy, 1, sides=sides, collective_id=3)
        w_g1, w_u1 = everywhere(update(0, 1, g_g1)), everywhere(update(1, 1, g_u1))
        sides = [Sum(pieces[2], *by_rows(hid0, back, 7), (1, 6, 9))]
        d_gate, d_up, g = backward(back, gate, up, w_down, 0, sides=sides, collective_id=4)
        sides = [Spread(pieces[2], update(2, 0, g), (0, 3, 7, 13))]
        *both, p0, p1, p2 = by_columns(a0, (d_gate, d_up), sides=sides, collective_id=6)
        parts, ms, vs = tail(both[::2], both[1::2], [(weights[k], m[k], v[k]) for k in range(2)], pieces)
        for which in range(2):
            new[3 + which][0], new[6 + which][0] = ms[which], vs[which]
        whole = placed([*parts, (p0, p1, p2)], pieces, (w_g1, w_u1, w_d1))
        for i in range(3):
            new[i] = whole[i].reshape(weights[i].shape)
        return tuple(one if i < 3 else jnp.stack(one) for i, one in enumerate(new))

    seq = P(("rep", "dp"), None, None)
    full = P(None, None, None)
    block = P(None, "dp", None)
    return jax.shard_map(
        body,
        mesh=mesh,
        in_specs=(seq, seq, *[full] * 3, *[block] * 6),
        out_specs=(*[P("rep", None, None)] * 3, *[P("rep", "dp", None)] * 6),
        check_vma=False,
    )
```
